128 devices in a mesh: batch: 16 (over y, x), cols: 8 (over z, core).
Axes of the slice: x: 4, y: 4, z: 4, core: 2. Of those that a mesh axis runs over, the one named last changes fastest.
Arguments:
- grad_up: float32 [16, 1024, 4096], P('batch', None, 'cols'), may hold values from -0.875 to 0.875
- grad_down: float32 [16, 4096, 1024], P('batch', 'cols'), may hold values from -0.875 to 0.875
- grad_query: float32 [16, 1024, 1024], P('batch', None, 'cols'), may hold values from -0.875 to 0.875
- grad_key: float32 [16, 1024, 1024], P('batch', None, 'cols'), may hold values from -0.875 to 0.875
- grad_value: float32 [16, 1024, 1024], P('batch', None, 'cols'), may hold values from -0.875 to 0.875
- grad_mixed: float32 [16, 1024, 1024], P('batch', 'cols'), may hold values from -0.875 to 0.875
- grad_norm: float32 [16, 1024], P('batch'), may hold values from -8 to 8
- weight_up: float32 [1024, 4096], P('batch', 'cols'), may hold values from -0.1875 to 0.1875
- weight_down: float32 [4096, 1024], P('cols', 'batch'), may hold values from -0.09375 to 0.09375
- weight_query: float32 [1024, 1024], P('batch', 'cols'), may hold values from -0.1875 to 0.1875
- weight_key: float32 [1024, 1024], P('batch', 'cols'), may hold values from -0.1875 to 0.1875
- weight_value: float32 [1024, 1024], P('batch', 'cols'), may hold values from -0.1875 to 0.1875
- weight_mixed: float32 [1024, 1024], P('cols', 'batch'), may hold values from -0.1875 to 0.1875
- weight_norm: float32 [1024], P('batch'), may hold values from 0.25 to 1.75
- moment_up: float32 [1024, 4096], P('batch', 'cols'), may hold values from -1.75 to 1.75
- moment_down: float32 [4096, 1024], P('cols', 'batch'), may hold values from -1.75 to 1.75
- moment_query: float32 [1024, 1024], P('batch', 'cols'), may hold values from -1.75 to 1.75
- moment_key: float32 [1024, 1024], P('batch', 'cols'), may hold values from -1.75 to 1.75
- moment_value: float32 [1024, 1024], P('batch', 'cols'), may hold values from -1.75 to 1.75
- moment_mixed: float32 [1024, 1024], P('cols', 'batch'), may hold values from -1.75 to 1.75
- moment_norm: float32 [1024], P('batch'), may hold values from -1.75 to 1.75
Outputs:
- copy_up: bfloat16 [1024, 4096], P(None, 'cols')
- copy_down: bfloat16 [4096, 1024], P('cols')
- copy_query: bfloat16 [1024, 1024], P(None, 'cols')
- copy_key: bfloat16 [1024, 1024], P(None, 'cols')
- copy_value: bfloat16 [1024, 1024], P(None, 'cols')
- copy_mixed: bfloat16 [1024, 1024], P('cols')
- copy_norm: bfloat16 [1024], replicated
- new_up: float32 [1024, 4096], P('batch', 'cols')
- new_down: float32 [4096, 1024], P('cols', 'batch')
- new_query: float32 [1024, 1024], P('batch', 'cols')
- new_key: float32 [1024, 1024], P('batch', 'cols')
- new_value: float32 [1024, 1024], P('batch', 'cols')
- new_mixed: float32 [1024, 1024], P('cols', 'batch')
- new_norm: float32 [1024], P('batch')
- state_new_up: float32 [1024, 4096], P('batch', 'cols')
- state_new_down: float32 [4096, 1024], P('cols', 'batch')
- state_new_query: float32 [1024, 1024], P('batch', 'cols')
- state_new_key: float32 [1024, 1024], P('batch', 'cols')
- state_new_value: float32 [1024, 1024], P('batch', 'cols')
- state_new_mixed: float32 [1024, 1024], P('cols', 'batch')
- state_new_norm: float32 [1024], P('batch')
The draws below stay inside these ranges and needn't reach their ends.
All inputs are finite; a program needn't handle non-finite values.
Results may differ from the reference program's by a relative error of at most 0.008.
Values may be sent and summed in bfloat16 or wider, within the bound.
A program may use at most 64 MiB of HBM per device.

```python
import jax
import jax.numpy as jnp

WIDTH = 1024
INNER = 4096
ATTN = 1024
REPLICAS = 16


def spiked(entries, rng, source, target, blocks, factor):
    owner, partner = [(jnp.arange(entries.shape[dim]) // (entries.shape[dim] // blocks)).reshape([-1 if axis == dim else 1 for axis in range(entries.ndim)]) for dim in (source, target)]
    chosen = jax.random.permutation(rng, blocks)[partner]
    strong = (owner == chosen) | (owner == (partner + blocks // 2) % blocks)
    return jnp.where(strong, factor * entries, entries)


def steps_of(rng, dims, cuts, smallest, top_value):
    level = 1.0
    for dim, parts in cuts:
        heights = jax.random.uniform(jax.random.fold_in(jax.random.fold_in(rng, 6), dim), (parts,), jnp.float32, smallest / len(cuts), top_value / len(cuts))
        level = level * jnp.repeat(jnp.exp(heights), dims[dim] // parts).reshape((-1,) + (1,) * (len(dims) - 1 - dim))
    return level


def centred(key, shape, scale, bound, pieces=(), kind=jnp.bfloat16):
    loudness = steps_of(key, shape, pieces, -0.22, 0.18) if pieces else 1.0
    drawn = jax.random.normal(key, shape, jnp.float32) * scale * loudness
    return jnp.minimum(jnp.maximum(drawn, -bound), bound).astype(kind)


def bell_draw_with(own_key, shape, deviation, most, split, heavy, kind=jnp.bfloat16):
    array = deviation * jax.random.normal(own_key, shape, jnp.float32)
    if split:
        array = array * steps_of(own_key, shape, split, -0.22, 0.18)
    return jnp.clip(spiked(array, jax.random.fold_in(own_key, 3), *heavy), -most, most).astype(kind)


def setup_inputs(seed: int = 0) -> dict:
    arg_keys = jax.random.split(jax.random.key(seed), 22)
    return {
        "grad_up": bell_draw_with(arg_keys[0], (REPLICAS, WIDTH, INNER), 0.1, 0.875, ((0, 16), (2, 8)), (0, 1, 16, 2.0), jnp.float32),
        "grad_down": bell_draw_with(arg_keys[1], (REPLICAS, INNER, WIDTH), 0.1, 0.875, ((0, 16), (1, 8)), (0, 2, 16, 2.0), jnp.float32),
        "grad_query": bell_draw_with(arg_keys[2], (REPLICAS, WIDTH, ATTN), 0.1, 0.875, ((0, 16), (2, 8)), (0, 1, 16, 2.0), jnp.float32),
        "grad_key": bell_draw_with(arg_keys[3], (REPLICAS, WIDTH, ATTN), 0.1, 0.875, ((0, 16), (2, 8)), (0, 1, 16, 2.0), jnp.float32),
        "grad_value": bell_draw_with(arg_keys[4], (REPLICAS, WIDTH, ATTN), 0.1, 0.875, ((0, 16), (2, 8)), (0, 1, 16, 2.0), jnp.float32),
        "grad_mixed": bell_draw_with(arg_keys[5], (REPLICAS, ATTN, WIDTH), 0.1, 0.875, ((0, 16), (1, 8)), (0, 2, 16, 2.0), jnp.float32),
        "grad_norm": bell_draw_with(arg_keys[6], (REPLICAS, WIDTH), 1.0, 8.0, ((0, 16),), (0, 1, 16, 2.0), jnp.float32),
        "weight_up": centred(arg_keys[7], (WIDTH, INNER), WIDTH ** -0.5, 0.1875, ((0, 16), (1, 8)), jnp.float32),
        "weight_down": centred(arg_keys[8], (INNER, WIDTH), INNER ** -0.5, 0.09375, ((0, 8), (1, 16)), jnp.float32),
        "weight_query": centred(arg_keys[9], (WIDTH, ATTN), WIDTH ** -0.5, 0.1875, ((0, 16), (1, 8)), jnp.float32),
        "weight_key": centred(arg_keys[10], (WIDTH, ATTN), WIDTH ** -0.5, 0.1875, ((0, 16), (1, 8)), jnp.float32),
        "weight_value": centred(arg_keys[11], (WIDTH, ATTN), WIDTH ** -0.5, 0.1875, ((0, 16), (1, 8)), jnp.float32),
        "weight_mixed": centred(arg_keys[12], (ATTN, WIDTH), ATTN ** -0.5, 0.1875, ((0, 8), (1, 16)), jnp.float32),
        "weight_norm": jnp.clip(1.0 + 0.15 * jax.random.normal(arg_keys[13], (WIDTH,), jnp.float32), 0.25, 1.75),
        "moment_up": centred(arg_keys[14], (WIDTH, INNER), 0.3, 1.75, ((0, 16), (1, 8)), jnp.float32),
        "moment_down": centred(arg_keys[15], (INNER, WIDTH), 0.3, 1.75, ((0, 8), (1, 16)), jnp.float32),
        "moment_query": centred(arg_keys[16], (WIDTH, ATTN), 0.3, 1.75, ((0, 16), (1, 8)), jnp.float32),
        "moment_key": centred(arg_keys[17], (WIDTH, ATTN), 0.3, 1.75, ((0, 16), (1, 8)), jnp.float32),
        "moment_value": centred(arg_keys[18], (WIDTH, ATTN), 0.3, 1.75, ((0, 16), (1, 8)), jnp.float32),
        "moment_mixed": centred(arg_keys[19], (ATTN, WIDTH), 0.3, 1.75, ((0, 8), (1, 16)), jnp.float32),
        "moment_norm": centred(arg_keys[20], (WIDTH,), 0.3, 1.75, ((0, 16),), jnp.float32),
    }


learn_rate = 0.1
hold_rate = 0.7


def reference(grad_up, grad_down, grad_query, grad_key, grad_value, grad_mixed, grad_norm, weight_up, weight_down, weight_query, weight_key, weight_value, weight_mixed, weight_norm, moment_up, moment_down, moment_query, moment_key, moment_value, moment_mixed, moment_norm):
    mean_up = jnp.sum(grad_up.astype(jnp.float32), axis=0) * REPLICAS ** -0.5
    mean_down = jnp.sum(grad_down.astype(jnp.float32), axis=0) * REPLICAS ** -0.5
    mean_query = jnp.sum(grad_query.astype(jnp.float32), axis=0) * REPLICAS ** -0.5
    mean_key = jnp.sum(grad_key.astype(jnp.float32), axis=0) * REPLICAS ** -0.5
    mean_value = jnp.sum(grad_value.astype(jnp.float32), axis=0) * REPLICAS ** -0.5
    mean_mixed = jnp.sum(grad_mixed.astype(jnp.float32), axis=0) * REPLICAS ** -0.5
    mean_norm = jnp.sum(grad_norm.astype(jnp.float32), axis=0) * REPLICAS ** -0.5
    state_new_up = hold_rate * moment_up + mean_up
    new_up = weight_up - learn_rate * state_new_up
    state_new_down = hold_rate * moment_down + mean_down
    new_down = weight_down - learn_rate * state_new_down
    state_new_query = hold_rate * moment_query + mean_query
    new_query = weight_query - learn_rate * state_new_query
    state_new_key = hold_rate * moment_key + mean_key
    new_key = weight_key - learn_rate * state_new_key
    state_new_value = hold_rate * moment_value + mean_value
    new_value = weight_value - learn_rate * state_new_value
    state_new_mixed = hold_rate * moment_mixed + mean_mixed
    new_mixed = weight_mixed - learn_rate * state_new_mixed
    state_new_norm = hold_rate * moment_norm + mean_norm
    new_norm = weight_norm - learn_rate * state_new_norm
    copy_up = new_up.astype(jnp.bfloat16)
    copy_down = new_down.astype(jnp.bfloat16)
    copy_query = new_query.astype(jnp.bfloat16)
    copy_key = new_key.astype(jnp.bfloat16)
    copy_value = new_value.astype(jnp.bfloat16)
    copy_mixed = new_mixed.astype(jnp.bfloat16)
    copy_norm = new_norm.astype(jnp.bfloat16)
    return copy_up, copy_down, copy_query, copy_key, copy_value, copy_mixed, copy_norm, new_up, new_down, new_query, new_key, new_value, new_mixed, new_norm, state_new_up, state_new_down, state_new_query, state_new_key, state_new_value, state_new_mixed, state_new_norm
```

```python
import jax
import jax.numpy as jnp
from jax import lax
from jax.experimental import pallas as pl
from jax.experimental.pallas import tpu as pltpu
from jax.sharding import PartitionSpec as P

learn_rate = 0.1
hold_rate = 0.7

SIDE = 4
LANES = 128
ROWS = 64
NAMES = ("up", "down", "query", "key", "value", "mixed")
ROW_CUT = ("up", "query", "key", "value")

PIECES = (
    (("up", 0), ("up", 1), ("up", 2), ("up", 3), ("query", 0), ("key", 0)),
    (("value", 0), ("mixed", 0), ("down", 0), ("down", 1), ("down", 2), ("down", 3)),
)
SEGMENTS = (1, 1, 1, 1, 1, 1)
HALF_ROWS = ROWS * 6
AXES = (("y", "x"), ("x", "y"))
F32, BF16 = jnp.float32, jnp.bfloat16


def low_lanes(shape):
    return lax.broadcasted_iota(jnp.int32, shape, len(shape) - 1) < LANES // 2


def swap_sides(value):
    return pltpu.roll(value, LANES // 2, len(value.shape) - 1)


def interleave(first, second):
    low = low_lanes(first.shape)
    return jnp.where(low, first, swap_sides(second)), jnp.where(low, swap_sides(first), second)


def segment_spans():
    spans, at = [], 0
    for count in SEGMENTS:
        spans.append((at, count))
        at += count
    return spans


def count_remote():
    return 2 * len(SEGMENTS) * 20 + 6


def exchange_kernel(*refs):
    refs = list(refs)

    def take(count):
        got, refs[:] = refs[:count], refs[count:]
        return got

    grad = dict(zip(NAMES, take(6)))
    (grad_norm,) = take(1)
    weight = dict(zip(NAMES, take(6)))
    (weight_norm,) = take(1)
    moment = dict(zip(NAMES, take(6)))
    (moment_norm,) = take(1)
    full = take(2)
    full_down, full_mixed = take(2)
    new_rows, state_rows = take(2), take(2)
    new_down, state_down, new_mixed, state_mixed = take(4)
    copy_norm, new_norm, state_norm = take(3)
    landed = take(2)
    packed, part = take(2), take(2)
    from_1, from_2 = take(2), take(2)
    weight_in = dict(zip(NAMES, take(6)))
    moment_in = dict(zip(NAMES, take(6)))
    weight_packed, moment_packed = take(2), take(2)
    norm_grad_in, norm_weight_in, norm_moment_in, norm_tiles = take(4)
    load_sem, send_sem, recv_sem = take(3)
    assert not refs

    me = lax.axis_index("batch")
    here = {"y": lax.div(me, SIDE), "x": lax.rem(me, SIDE)}
    step = {a: {d: lax.rem(here[a] + d + SIDE, SIDE) for d in (-1, 1, 2)} for a in ("y", "x")}

    def device(axis, d):
        at = dict(here)
        at[axis] = step[axis][d]
        return {"batch": at["y"] * SIDE + at["x"]}

    barrier = pltpu.get_barrier_semaphore()
    for axis in ("y", "x"):
        for d in (-1, 1):
            pl.semaphore_signal(barrier, inc=1, device_id=device(axis, d), device_id_type=pl.DeviceIdType.MESH)

    loads = {}

    def load(key, source, target):
        copy = pltpu.make_async_copy(source, target, load_sem.at[len(loads)])
        copy.start()
        loads[key] = copy

    for k in range(6):
        for half in (0, 1):
            name, part_no = PIECES[half][k]
            if name in ROW_CUT:
                load((half, k), grad[name].at[0, :, pl.ds(part_no * LANES, LANES)], landed[0].at[slot_of(half, k)])
            else:
                load((half, k), grad[name].at[0, pl.ds(part_no * LANES, LANES), :], landed[1].at[slot_of(half, k)])
        if k == 0:
            load("norm_grad", grad_norm, norm_grad_in)
            load("norm_weight", weight_norm, norm_weight_in)
            load("norm_moment", moment_norm, norm_moment_in)
    for name in NAMES:
        load(("weight", name), weight[name], weight_in[name])
        load(("moment", name), moment[name], moment_in[name])

    def pack_piece(half, k):
        name, part_no = PIECES[half][k]
        loads[half, k].wait()
        rows = pl.ds(k * ROWS, ROWS)
        slot = slot_of(half, k)

        def put(b, value):
            y, x = divmod(b, SIDE)
            at = (y, x) if AXES[half][0] == "y" else (x, y)
            packed[half][at[0], at[1], rows, :] = value.astype(BF16)

        if name in ROW_CUT:
            for b in range(SIDE * SIDE):
                put(b, landed[0][slot, b * ROWS : (b + 1) * ROWS, :])
        else:
            for m in range(SIDE * SIDE // 2):
                lanes = slice(m * LANES, (m + 1) * LANES)
                pair = interleave(landed[1][slot, :ROWS, lanes], landed[1][slot, ROWS:, lanes])
                put(2 * m, pair[0])
                put(2 * m + 1, pair[1])

    def pack_own():
        for half in (0, 1):
            for k, (name, part_no) in enumerate(PIECES[half]):
                rows = pl.ds(k * ROWS, ROWS)
                if part_no == 0:
                    loads["weight", name].wait()
                    loads["moment", name].wait()
                for source, target in ((weight_in[name], weight_packed[half]), (moment_in[name], moment_packed[half])):
                    if name in ROW_CUT:
                        target[rows, :] = source[:, part_no * LANES : (part_no + 1) * LANES]
                    else:
                        turned = source[:, part_no * LANES : (part_no + 1) * LANES].T
                        target[rows, :] = jnp.concatenate([turned[:ROWS, :], turned[ROWS:, :]], axis=1)

    sent = {}

    def send(key, source, target, axis, d):
        n = len(sent)
        copy = pltpu.make_async_remote_copy(
            src_ref=source,
            dst_ref=target,
            send_sem=send_sem.at[n],
            recv_sem=recv_sem.at[n],
            device_id=device(axis, d),
            device_id_type=pl.DeviceIdType.MESH,
        )
        copy.start()
        sent[key] = copy

    def arrived(key):
        sent[key].wait_recv()

    def spans(s):
        at, count = segment_spans()[s]
        rows, side = at * ROWS, count * ROWS // 2
        return (pl.ds(rows, side), pl.ds(rows + side, side), pl.ds(rows // 2, side), pl.ds(rows, 2 * side))

    def reduce_send(half, level, s):
        axis = AXES[half][level]
        low, high, place, _ = spans(s)
        data = (packed, part)[level][half]
        land = (from_1, from_2)[level][half]

        def src(d, rows):
            return data.at[step[axis][d], :, rows, :] if level == 0 else data.at[step[axis][d], rows, :]

        def dst(kind, d):
            return land.at[kind, 0 if d == 1 else 1, :, place, :] if level == 0 else land.at[kind, 0 if d == 1 else 1, place, :]

        send((half, level, s, 0, 1), src(2, low), dst(0, 1), axis, 1)
        send((half, level, s, 0, -1), src(2, high), dst(0, -1), axis, -1)
        send((half, level, s, 1, 1), src(1, high), dst(1, 1), axis, 1)
        send((half, level, s, 1, -1), src(-1, low), dst(1, -1), axis, -1)

    def reduce_forward(half, level, s):
        axis = AXES[half][level]
        low, high, place, _ = spans(s)
        data = (packed, part)[level][half]
        land = (from_1, from_2)[level][half]
        for d, rows in ((1, low), (-1, high)):
            arrived((half, level, s, 0, d))
            side = 0 if d == 1 else 1
            to = step[axis][d]
            if level == 0:
                total = data[to, :, rows, :].astype(F32) + land[0, side, :, place, :].astype(F32)
                data[to, :, rows, :] = total.astype(BF16)
                send((half, level, s, 2, d), data.at[to, :, rows, :], land.at[2, side, :, place, :], axis, d)
            else:
                total = data[to, rows, :].astype(F32) + land[0, side, place, :].astype(F32)
                data[to, rows, :] = total.astype(BF16)
                send((half, level, s, 2, d), data.at[to, rows, :], land.at[2, side, place, :], axis, d)

    def reduce_totals(half, level, s):
        axis = AXES[half][level]
        low, high, place, _ = spans(s)
        data = (packed, part)[level][half]
        land = (from_1, from_2)[level][half]
        arrived((half, level, s, 1, 1))
        arrived((half, level, s, 1, -1))
        arrived((half, level, s, 2, 1))
        arrived((half, level, s, 2, -1))
        mine = here[axis]
        for rows, (first, second) in ((low, ((2, 0), (1, 1))), (high, ((1, 0), (2, 1)))):
            if level == 0:
                total = data[mine, :, rows, :].astype(F32)
                total += land[first[0], first[1], :, place, :].astype(F32)
                total += land[second[0], second[1], :, place, :].astype(F32)
            else:
                total = data[mine, rows, :].astype(F32)
                total += land[first[0], first[1], place, :].astype(F32)
                total += land[second[0], second[1], place, :].astype(F32)
            yield rows, total

    def first_totals(half, s):
        for rows, total in reduce_totals(half, 0, s):
            part[half][:, rows, :] = total.astype(BF16)

    mean_rate = float(SIDE * SIDE) ** -0.5

    def update(half, s):
        first, second = AXES[half]
        for rows, total in reduce_totals(half, 1, s):
            state = hold_rate * moment_packed[half][rows, :] + total * mean_rate
            new = weight_packed[half][rows, :] - learn_rate * state
            state_rows[half][rows, :] = state
            new_rows[half][rows, :] = new
            full[half][here[first], here[second], rows, :] = new.astype(BF16)
        at, count = segment_spans()[s]
        for k in range(at, at + count):
            name, part_no = PIECES[half][k]
            if name in ROW_CUT:
                continue
            rows = pl.ds(k * ROWS, ROWS)
            targets = (new_down, state_down) if name == "down" else (new_mixed, state_mixed)
            for source, target in zip((new_rows[half], state_rows[half]), targets):
                turned = source[rows, :].T
                target[:, part_no * LANES : (part_no + 1) * LANES] = jnp.concatenate([turned[:ROWS, :], turned[ROWS:, :]], axis=1)

    def gather_part(half, level, d, rows):
        first, second = AXES[half]
        if level == 1:
            at = here[second] if d == 0 else step[second][d]
            return full[half].at[here[first], at, rows, :]
        at = here[first] if d == 0 else step[first][d]
        return full[half].at[at, :, rows, :]

    def gather_send(half, level, s):
        whole = spans(s)[3]
        axis = AXES[half][level]
        block = gather_part(half, level, 0, whole)
        for d in (1, -1):
            send((half, level, s, 3, d), block, block, axis, d)

    def gather_forward(half, level, s):
        low, high, _, _ = spans(s)
        axis = AXES[half][level]
        for d, rows in ((1, low), (-1, high)):
            arrived((half, level, s, 3, d))
            block = gather_part(half, level, -d, rows)
            send((half, level, s, 4, d), block, block, axis, d)

    def gather_end(half, level, s):
        arrived((half, level, s, 4, 1))
        arrived((half, level, s, 4, -1))

    def unpack(half, s):
        at, count = segment_spans()[s]
        for k in range(at, at + count):
            name, part_no = PIECES[half][k]
            if name in ROW_CUT:
                continue
            target = full_down if name == "down" else full_mixed
            rows = pl.ds(k * ROWS, ROWS)
            for m in range(SIDE * SIDE // 2):
                pair = []
                for b in (2 * m, 2 * m + 1):
                    y, x = divmod(b, SIDE)
                    at_ = (y, x) if AXES[half][0] == "y" else (x, y)
                    pair.append(full[half][at_[0], at_[1], rows, :].astype(F32))
                top, bottom = interleave(*pair)
                lanes = slice(m * LANES, (m + 1) * LANES)
                target[part_no * LANES : part_no * LANES + ROWS, lanes] = top.astype(BF16)
                target[part_no * LANES + ROWS : (part_no + 1) * LANES, lanes] = bottom.astype(BF16)

    def norm_start():
        for key in ("norm_grad", "norm_weight", "norm_moment"):
            loads[key].wait()
        for k in range(8):
            norm_tiles[0, k : k + 1, :] = norm_grad_in[0:1, k * LANES : (k + 1) * LANES]
        base = norm_weight_in[...] - learn_rate * (hold_rate * norm_moment_in[...])
        base = jnp.broadcast_to(jnp.concatenate([base, base], axis=1), (8, LANES))
        row = lax.broadcasted_iota(jnp.int32, (8, LANES), 0)
        owner = 2 * row + jnp.where(low_lanes((8, LANES)), 0, 1)
        norm_tiles[0, 8:16, :] = jnp.where(owner == me, base, 0.0)
        norm_send("y", 0)

    def norm_send(axis, at):
        for d in (1, -1):
            send(("norm", axis, d), norm_tiles.at[at], norm_tiles.at[at + (1 if d == 1 else 2)], axis, d)

    def norm_forward(axis, at):
        arrived(("norm", axis, 1))
        send(("norm", axis, 2), norm_tiles.at[at + 1], norm_tiles.at[at + 3], axis, 1)

    def norm_total(axis, at):
        arrived(("norm", axis, -1))
        arrived(("norm", axis, 2))
        return (norm_tiles[at] + norm_tiles[at + 1]) + (norm_tiles[at + 2] + norm_tiles[at + 3])

    def norm_middle():
        norm_tiles[4] = norm_total("y", 0)
        norm_send("x", 4)

    def norm_end():
        total = norm_total("x", 4)
        mean = total[0:8, :] * mean_rate
        norm_tiles[8, 0:8, :] = mean
        new = (total[8:16, :] - learn_rate * mean).astype(BF16)
        for k in range(8):
            copy_norm[0:1, k * LANES : (k + 1) * LANES] = new[k : k + 1, :]
        own = norm_tiles[8, pl.ds(lax.div(me, 2), 1), :]
        own = jnp.where(lax.rem(me, 2) == 1, swap_sides(own), own)[:, : LANES // 2]
        state = hold_rate * norm_moment_in[...] + own
        state_norm[...] = state
        new_norm[...] = norm_weight_in[...] - learn_rate * state

    def begin(half, s):
        at, count = segment_spans()[s]
        for k in range(at, at + count):
            pack_piece(half, k)
        if half == 0 and s == 0:
            pl.semaphore_wait(barrier, 4)
        reduce_send(half, 0, s)

    def second_send(half, s):
        first_totals(half, s)
        reduce_send(half, 1, s)

    def share(half, s):
        update(half, s)
        gather_send(half, 1, s)

    def second_share(half, s):
        gather_end(half, 1, s)
        gather_send(half, 0, s)

    def finish(half, s):
        gather_end(half, 0, s)
        unpack(half, s)

    stages = (
        begin,
        lambda half, s: reduce_forward(half, 0, s),
        second_send,
        lambda half, s: reduce_forward(half, 1, s),
        share,
        lambda half, s: gather_forward(half, 1, s),
        second_share,
        lambda half, s: gather_forward(half, 0, s),
        finish,
    )
    count = len(SEGMENTS)
    for t in range(count + len(stages) - 1):
        for n, stage in enumerate(stages):
            if 0 <= t - n < count:
                for half in (0, 1):
                    stage(half, t - n)
        if t == 0:
            norm_start()
            pack_own()
        if t == 2:
            norm_forward("y", 0)
        if t == 3:
            norm_middle()
        if t == 5:
            norm_forward("x", 4)
        if t == 7:
            norm_end()
    for copy in sent.values():
        copy.wait_send()


def slot_of(half, k):
    order = [p for h in (0, 1) for p in PIECES[h]]
    this = PIECES[half][k]
    kind = this[0] in ROW_CUT
    return [p for p in order if (p[0] in ROW_CUT) == kind].index(this)


def place_kernel(*refs):
    refs = list(refs)

    def take(count):
        got, refs[:] = refs[:count], refs[count:]
        return got

    full = take(2)
    full_down, full_mixed = take(2)
    new_rows, state_rows = take(2), take(2)
    new_down_in, state_down_in, new_mixed_in, state_mixed_in = take(4)
    norms_in = take(3)
    copy_out = dict(zip(ROW_CUT, take(4)))
    copy_down, copy_mixed = take(2)
    new_out = dict(zip(ROW_CUT, take(4)))
    new_down, new_mixed = take(2)
    state_out = dict(zip(ROW_CUT, take(4)))
    state_down, state_mixed = take(2)
    norms_out = take(3)
    (sem,) = take(1)
    assert not refs
    copies = []

    def put(source, target):
        copies.append(pltpu.make_async_copy(source, target, sem.at[len(copies)]))
        copies[-1].start()

    for half in (0, 1):
        for k, (name, part_no) in enumerate(PIECES[half]):
            if name not in ROW_CUT:
                continue
            rows, lanes = pl.ds(k * ROWS, ROWS), pl.ds(part_no * LANES, LANES)
            if AXES[half][0] == "y":
                put(full[half].at[:, :, rows, :], copy_out[name].at[:, :, :, lanes])
            else:
                for n in range(SIDE):
                    put(full[half].at[n, :, rows, :], copy_out[name].at[:, n, :, lanes])
            put(new_rows[half].at[rows, :], new_out[name].at[:, lanes])
            put(state_rows[half].at[rows, :], state_out[name].at[:, lanes])
    put(full_down, copy_down)
    put(full_mixed, copy_mixed)
    put(new_down_in, new_down)
    put(state_down_in, state_down)
    put(new_mixed_in, new_mixed)
    put(state_mixed_in, state_mixed)
    for source, target in zip(norms_in, norms_out):
        put(source, target)
    for copy in copies:
        copy.wait()


PLACE_COPIES = 2 + 4 + 6 * 2 + 4 + 4 + 2 * 7 + 3


def in_hbm(arrays):
    return [pltpu.with_memory_space_constraint(a, pltpu.HBM) for a in arrays]


def body(*arrays):
    arrays = [a.T if a.ndim == 2 and a.shape[1] == ROWS else a for a in arrays]
    grads, weights, moments = arrays[:7], arrays[7:14], arrays[14:]
    shapes = [w.shape for w in weights[:6]]
    half = jax.ShapeDtypeStruct((SIDE, SIDE, HALF_ROWS, LANES), BF16)
    rows = jax.ShapeDtypeStruct((HALF_ROWS, LANES), F32)
    down, mixed = jax.ShapeDtypeStruct(shapes[1], F32), jax.ShapeDtypeStruct(shapes[5], F32)
    held = (
        half,
        half,
        jax.ShapeDtypeStruct(grads[1].shape[1:], BF16),
        jax.ShapeDtypeStruct(grads[5].shape[1:], BF16),
        rows,
        rows,
        rows,
        rows,
        down,
        down,
        mixed,
        mixed,
        jax.ShapeDtypeStruct((1, 8 * LANES), BF16),
        jax.ShapeDtypeStruct((1, LANES // 2), F32),
        jax.ShapeDtypeStruct((1, LANES // 2), F32),
    )
    dma = pltpu.SemaphoreType.DMA
    remote = count_remote()
    vmem = pl.BlockSpec(memory_space=pltpu.VMEM)
    anywhere = pl.BlockSpec(memory_space=pltpu.HBM)
    half_scratch = pltpu.VMEM((SIDE, SIDE, HALF_ROWS, LANES), BF16)
    part_scratch = pltpu.VMEM((SIDE, HALF_ROWS, LANES), BF16)
    from_1 = pltpu.VMEM((3, 2, SIDE, HALF_ROWS // 2, LANES), BF16)
    from_2 = pltpu.VMEM((3, 2, HALF_ROWS // 2, LANES), BF16)
    own = [pltpu.VMEM(s, F32) for s in shapes]
    own_packed = pltpu.VMEM((HALF_ROWS, LANES), F32)
    small = pltpu.VMEM((1, LANES // 2), F32)
    results = pl.pallas_call(
        exchange_kernel,
        out_shape=held,
        in_specs=[anywhere] * 21,
        out_specs=[vmem] * len(held),
        scratch_shapes=[
            pltpu.VMEM((7, SIDE * SIDE * ROWS, LANES), F32),
            pltpu.VMEM((5, LANES, SIDE * SIDE * ROWS), F32),
            half_scratch,
            half_scratch,
            part_scratch,
            part_scratch,
            from_1,
            from_1,
            from_2,
            from_2,
            *own,
            *own,
            own_packed,
            own_packed,
            own_packed,
            own_packed,
            pltpu.VMEM((1, 8 * LANES), F32),
            small,
            small,
            pltpu.VMEM((9, 16, LANES), F32),
            dma((27,)),
            dma((remote,)),
            dma((remote,)),
        ],
        compiler_params=pltpu.CompilerParams(
            collective_id=0, has_side_effects=True, vmem_limit_bytes=32 * 1024 * 1024
        ),
        name="exchange",
    )(
        *in_hbm(grads),
        *in_hbm(weights[:6]),
        *in_hbm([weights[6].reshape(1, -1)]),
        *in_hbm(moments[:6]),
        *in_hbm([moments[6].reshape(1, -1)]),
    )
    row_shapes = [shapes[NAMES.index(n)] for n in ROW_CUT]
    tall = [jax.ShapeDtypeStruct((SIDE, SIDE, *s), BF16) for s in row_shapes]
    own_rows = [jax.ShapeDtypeStruct(s, F32) for s in row_shapes]
    placed = pl.pallas_call(
        place_kernel,
        out_shape=(*tall, held[2], held[3], *own_rows, down, mixed, *own_rows, down, mixed, *held[12:]),
        in_specs=[vmem] * 15,
        out_specs=[anywhere] * 21,
        scratch_shapes=[dma((PLACE_COPIES,))],
        compiler_params=pltpu.CompilerParams(vmem_limit_bytes=16 * 1024 * 1024),
        name="place",
    )(*results)
    outs = []
    for k, last in zip((0, 6, 12), placed[18:]):
        up, query, key, value, down_, mixed_ = placed[k : k + 6]
        group = [up, down_, query, key, value, mixed_]
        if k == 0:
            group = [g.reshape(-1, g.shape[-1]) for g in group]
        else:
            group[1], group[5] = group[1].T, group[5].T
        outs += [*group, last.reshape(-1)]
    return tuple(outs)


def solution(mesh):
    cut_rows, cut_columns = P("batch", "cols"), P("cols", "batch")
    own = (cut_rows, cut_columns, cut_rows, cut_rows, cut_rows, cut_columns, P("batch"))
    grad_rows, grad_columns = P("batch", None, "cols"), P("batch", "cols", None)
    grads = (grad_rows, grad_columns, grad_rows, grad_rows, grad_rows, grad_columns, P("batch", None))
    whole_rows, whole_columns = P(None, "cols"), P("cols", None)
    copies = (whole_rows, whole_columns, whole_rows, whole_rows, whole_rows, whole_columns, P())
    return jax.shard_map(
        body, mesh=mesh, in_specs=(*grads, *own, *own), out_specs=(*copies, *own, *own), check_vma=False
    )
```

```python
import jax
import jax.numpy as jnp
from jax import lax
from jax.experimental import pallas as pl
from jax.experimental.pallas import tpu as pltpu
from jax.sharding import PartitionSpec as P

learn_rate = 0.1
hold_rate = 0.7

SIDE = 4
LANES = 128
ROWS = 64
NAMES = ("up", "down", "query", "key", "value", "mixed")
ROW_CUT = ("up", "query", "key", "value")

PIECES = (
    (("up", 0), ("up", 1), ("up", 2), ("up", 3), ("query", 0), ("key", 0)),
    (("value", 0), ("mixed", 0), ("down", 0), ("down", 1), ("down", 2), ("down", 3)),
)
SEGMENTS = (2, 3, 1)
HALF_ROWS = ROWS * 6
AXES = (("y", "x"), ("x", "y"))
AWAY = (1, -1, 2)
F32, BF16 = jnp.float32, jnp.bfloat16


def low_lanes(shape):
    return lax.broadcasted_iota(jnp.int32, shape, len(shape) - 1) < LANES // 2


def swap_sides(value):
    return pltpu.roll(value, LANES // 2, len(value.shape) - 1)


def interleave(first, second):
    low = low_lanes(first.shape)
    return jnp.where(low, first, swap_sides(second)), jnp.where(low, swap_sides(first), second)


def segment_spans():
    spans, at = [], 0
    for count in SEGMENTS:
        spans.append((at, count))
        at += count
    return spans


def count_remote():
    return 2 * len(SEGMENTS) * 16 + 6


def exchange_kernel(*refs):
    refs = list(refs)

    def take(count):
        got, refs[:] = refs[:count], refs[count:]
        return got

    grad = dict(zip(NAMES, take(6)))
    (grad_norm,) = take(1)
    weight = dict(zip(NAMES, take(6)))
    (weight_norm,) = take(1)
    moment = dict(zip(NAMES, take(6)))
    (moment_norm,) = take(1)
    full = take(2)
    full_down, full_mixed = take(2)
    new_rows, state_rows = take(2), take(2)
    new_down, state_down, new_mixed, state_mixed = take(4)
    copy_norm, new_norm, state_norm = take(3)
    landed = take(2)
    packed, part = take(2), take(2)
    from_1, from_2 = take(2), take(2)
    weight_in = dict(zip(NAMES, take(6)))
    moment_in = dict(zip(NAMES, take(6)))
    weight_packed, moment_packed = take(2), take(2)
    norm_grad_in, norm_weight_in, norm_moment_in, norm_tiles = take(4)
    load_sem, send_sem, recv_sem = take(3)
    assert not refs

    me = lax.axis_index("batch")
    here = {"y": lax.div(me, SIDE), "x": lax.rem(me, SIDE)}
    step = {a: {d: lax.rem(here[a] + d + SIDE, SIDE) for d in AWAY} for a in ("y", "x")}

    def device(axis, d):
        at = dict(here)
        at[axis] = step[axis][d]
        return {"batch": at["y"] * SIDE + at["x"]}

    loads = {}

    def load(key, source, target):
        copy = pltpu.make_async_copy(source, target, load_sem.at[len(loads)])
        copy.start()
        loads[key] = copy

    def load_segment(half, s):
        at, count = segment_spans()[s]
        for k in range(at, at + count):
            name, part_no = PIECES[half][k]
            lanes = pl.ds(part_no * LANES, LANES)
            if name in ROW_CUT:
                load((half, k), grad[name].at[0, :, lanes], landed[0].at[slot_of(half, k)])
            else:
                load((half, k), grad[name].at[0, lanes, :], landed[1].at[slot_of(half, k)])

    def load_own():
        load("norm_grad", grad_norm, norm_grad_in)
        load("norm_weight", weight_norm, norm_weight_in)
        load("norm_moment", moment_norm, norm_moment_in)
        for name in NAMES:
            load(("weight", name), weight[name], weight_in[name])
            load(("moment", name), moment[name], moment_in[name])

    for half in (0, 1):
        load_segment(half, 0)
    barrier = pltpu.get_barrier_semaphore()
    for axis in ("y", "x"):
        for d in AWAY:
            pl.semaphore_signal(barrier, inc=1, device_id=device(axis, d), device_id_type=pl.DeviceIdType.MESH)

    def pack_piece(half, k):
        name, part_no = PIECES[half][k]
        loads[half, k].wait()
        rows = pl.ds(k * ROWS, ROWS)
        slot = slot_of(half, k)

        def put(b, value):
            y, x = divmod(b, SIDE)
            at = (y, x) if AXES[half][0] == "y" else (x, y)
            packed[half][at[0], at[1], rows, :] = value.astype(BF16)

        if name in ROW_CUT:
            for b in range(SIDE * SIDE):
                put(b, landed[0][slot, b * ROWS : (b + 1) * ROWS, :])
        else:
            for m in range(SIDE * SIDE // 2):
                lanes = slice(m * LANES, (m + 1) * LANES)
                pair = interleave(landed[1][slot, :ROWS, lanes], landed[1][slot, ROWS:, lanes])
                put(2 * m, pair[0])
                put(2 * m + 1, pair[1])

    def pack_own():
        for half in (0, 1):
            for k, (name, part_no) in enumerate(PIECES[half]):
                rows = pl.ds(k * ROWS, ROWS)
                if part_no == 0:
                    loads["weight", name].wait()
                    loads["moment", name].wait()
                for source, target in ((weight_in[name], weight_packed[half]), (moment_in[name], moment_packed[half])):
                    if name in ROW_CUT:
                        target[rows, :] = source[:, part_no * LANES : (part_no + 1) * LANES]
                    else:
                        turned = source[:, part_no * LANES : (part_no + 1) * LANES].T
                        target[rows, :] = jnp.concatenate([turned[:ROWS, :], turned[ROWS:, :]], axis=1)

    sent = {}

    def send(key, source, target, axis, d):
        n = len(sent)
        copy = pltpu.make_async_remote_copy(
            src_ref=source,
            dst_ref=target,
            send_sem=send_sem.at[n],
            recv_sem=recv_sem.at[n],
            device_id=device(axis, d),
            device_id_type=pl.DeviceIdType.MESH,
        )
        copy.start()
        sent[key] = copy

    def arrived(key):
        sent[key].wait_recv()

    def spans(s):
        at, count = segment_spans()[s]
        rows, side = at * ROWS, count * ROWS // 2
        return (pl.ds(rows, side), pl.ds(rows + side, side), pl.ds(rows // 2, side), pl.ds(rows, 2 * side))

    def first_send(half, s):
        axis = AXES[half][0]
        low, high, place, _ = spans(s)
        data, land = packed[half], from_1[half]
        send((half, s, 0, 1), data.at[step[axis][2], :, low, :], land.at[0, 0, :, place, :], axis, 1)
        send((half, s, 0, -1), data.at[step[axis][2], :, high, :], land.at[0, 1, :, place, :], axis, -1)
        send((half, s, 1, 1), data.at[step[axis][1], :, high, :], land.at[1, 0, :, place, :], axis, 1)
        send((half, s, 1, -1), data.at[step[axis][-1], :, low, :], land.at[1, 1, :, place, :], axis, -1)

    def first_forward(half, s):
        axis = AXES[half][0]
        low, high, place, _ = spans(s)
        data, land = packed[half], from_1[half]
        for side, d, rows in ((0, 1, low), (1, -1, high)):
            arrived((half, s, 0, d))
            to = step[axis][d]
            total = data[to, :, rows, :].astype(F32) + land[0, side, :, place, :].astype(F32)
            data[to, :, rows, :] = total.astype(BF16)
            send((half, s, 2, d), data.at[to, :, rows, :], land.at[2, side, :, place, :], axis, d)

    def second_send(half, s):
        low, high, place, whole = spans(s)
        data, land = packed[half], from_1[half]
        for kind in (1, 2):
            for d in (1, -1):
                arrived((half, s, kind, d))
        mine = here[AXES[half][0]]
        for rows, first, second in ((low, 2, 1), (high, 1, 2)):
            total = data[mine, :, rows, :].astype(F32)
            total += land[first, 0, :, place, :].astype(F32)
            total += land[second, 1, :, place, :].astype(F32)
            part[half][:, rows, :] = total.astype(BF16)
        axis = AXES[half][1]
        for n, d in ((2, 2), (0, 1), (1, -1)):
            send((half, s, 3, d), part[half].at[step[axis][d], whole, :], from_2[half].at[n, whole, :], axis, d)

    mean_rate = float(SIDE * SIDE) ** -0.5

    def update(half, s):
        first, second = AXES[half]
        whole = spans(s)[3]
        for d in AWAY:
            arrived((half, s, 3, d))
        total = part[half][here[second], whole, :].astype(F32)
        for n in range(3):
            total += from_2[half][n, whole, :].astype(F32)
        state = hold_rate * moment_packed[half][whole, :] + total * mean_rate
        new = weight_packed[half][whole, :] - learn_rate * state
        state_rows[half][whole, :] = state
        new_rows[half][whole, :] = new
        full[half][here[first], here[second], whole, :] = new.astype(BF16)
        own = full[half].at[here[first], here[second], whole, :]
        for d in (2, 1, -1):
            send((half, s, 4, d), own, own, second, d)

    def turn_own(half, s):
        at, count = segment_spans()[s]
        for k in range(at, at + count):
            name, part_no = PIECES[half][k]
            if name in ROW_CUT:
                continue
            rows = pl.ds(k * ROWS, ROWS)
            targets = (new_down, state_down) if name == "down" else (new_mixed, state_mixed)
            for source, target in zip((new_rows[half], state_rows[half]), targets):
                turned = source[rows, :].T
                target[:, part_no * LANES : (part_no + 1) * LANES] = jnp.concatenate([turned[:ROWS, :], turned[ROWS:, :]], axis=1)

    def share(half, s):
        for d in AWAY:
            arrived((half, s, 4, d))
        first = AXES[half][0]
        block = full[half].at[here[first], :, spans(s)[3], :]
        for d in (1, -1):
            send((half, s, 5, d), block, block, first, d)
        turn_own(half, s)

    def share_forward(half, s):
        first = AXES[half][0]
        low, high, _, _ = spans(s)
        for d, rows in ((1, low), (-1, high)):
            arrived((half, s, 5, d))
            block = full[half].at[step[first][-d], :, rows, :]
            send((half, s, 6, d), block, block, first, d)

    def unpack(half, s):
        at, count = segment_spans()[s]
        for k in range(at, at + count):
            name, part_no = PIECES[half][k]
            if name in ROW_CUT:
                continue
            target = full_down if name == "down" else full_mixed
            rows = pl.ds(k * ROWS, ROWS)
            for m in range(SIDE * SIDE // 2):
                pair = []
                for b in (2 * m, 2 * m + 1):
                    y, x = divmod(b, SIDE)
                    at_ = (y, x) if AXES[half][0] == "y" else (x, y)
                    pair.append(full[half][at_[0], at_[1], rows, :].astype(F32))
                top, bottom = interleave(*pair)
                lanes = slice(m * LANES, (m + 1) * LANES)
                target[part_no * LANES : part_no * LANES + ROWS, lanes] = top.astype(BF16)
                target[part_no * LANES + ROWS : (part_no + 1) * LANES, lanes] = bottom.astype(BF16)

    def norm_start():
        for key in ("norm_grad", "norm_weight", "norm_moment"):
            loads[key].wait()
        for k in range(8):
            norm_tiles[0, k : k + 1, :] = norm_grad_in[0:1, k * LANES : (k + 1) * LANES]
        base = norm_weight_in[...] - learn_rate * (hold_rate * norm_moment_in[...])
        base = jnp.broadcast_to(jnp.concatenate([base, base], axis=1), (8, LANES))
        row = lax.broadcasted_iota(jnp.int32, (8, LANES), 0)
        owner = 2 * row + jnp.where(low_lanes((8, LANES)), 0, 1)
        norm_tiles[0, 8:16, :] = jnp.where(owner == me, base, 0.0)
        norm_send("y", 0)

    def norm_send(axis, at):
        for n, d in enumerate(AWAY):
            send(("norm", axis, d), norm_tiles.at[at], norm_tiles.at[at + 1 + n], axis, d)

    def norm_total(axis, at):
        for d in AWAY:
            arrived(("norm", axis, d))
        return (norm_tiles[at] + norm_tiles[at + 1]) + (norm_tiles[at + 2] + norm_tiles[at + 3])

    def norm_middle():
        norm_tiles[4] = norm_total("y", 0)
        norm_send("x", 4)

    def norm_end():
        total = norm_total("x", 4)
        mean = total[0:8, :] * mean_rate
        norm_tiles[8, 0:8, :] = mean
        new = (total[8:16, :] - learn_rate * mean).astype(BF16)
        for k in range(8):
            copy_norm[k * LANES : (k + 1) * LANES] = new[k, :]
        own = norm_tiles[8, pl.ds(lax.div(me, 2), 1), :]
        own = jnp.where(lax.rem(me, 2) == 1, swap_sides(own), own)[:, : LANES // 2]
        state = hold_rate * norm_moment_in[...] + own
        state_norm[...] = state
        new_norm[...] = norm_weight_in[...] - learn_rate * state

    def begin(half, s):
        at, count = segment_spans()[s]
        for k in range(at, at + count):
            pack_piece(half, k)
        if half == 0 and s == 0:
            pl.semaphore_wait(barrier, 2 * len(AWAY))
        first_send(half, s)
        if s + 1 < len(SEGMENTS):
            load_segment(half, s + 1)
        elif half == 1:
            load_own()

    def finish(half, s):
        for d in (1, -1):
            arrived((half, s, 6, d))
        unpack(half, s)

    stages = (begin, first_forward, second_send, update, share, share_forward, finish)
    after = {0: (norm_start,), 1: (norm_middle, pack_own), 2: (norm_end,)}
    for n, stage in enumerate(stages):
        for s in range(len(SEGMENTS)):
            for half in (0, 1):
                stage(half, s)
        for extra in after.get(n, ()):
            extra()
    for copy in sent.values():
        copy.wait_send()


def slot_of(half, k):
    order = [p for h in (0, 1) for p in PIECES[h]]
    this = PIECES[half][k]
    kind = this[0] in ROW_CUT
    return [p for p in order if (p[0] in ROW_CUT) == kind].index(this)


def place_kernel(*refs):
    refs = list(refs)

    def take(count):
        got, refs[:] = refs[:count], refs[count:]
        return got

    full = take(2)
    full_down, full_mixed = take(2)
    new_rows, state_rows = take(2), take(2)
    new_down_in, state_down_in, new_mixed_in, state_mixed_in = take(4)
    norms_in = take(3)
    copy_out = dict(zip(ROW_CUT, take(4)))
    copy_down, copy_mixed = take(2)
    new_out = dict(zip(ROW_CUT, take(4)))
    new_down, new_mixed = take(2)
    state_out = dict(zip(ROW_CUT, take(4)))
    state_down, state_mixed = take(2)
    norms_out = take(3)
    (sem,) = take(1)
    assert not refs
    copies = []

    def put(source, target):
        copies.append(pltpu.make_async_copy(source, target, sem.at[len(copies)]))
        copies[-1].start()

    for half in (0, 1):
        for k, (name, part_no) in enumerate(PIECES[half]):
            if name not in ROW_CUT:
                continue
            rows, lanes = pl.ds(k * ROWS, ROWS), pl.ds(part_no * LANES, LANES)
            if AXES[half][0] == "y":
                put(full[half].at[:, :, rows, :], copy_out[name].at[:, :, :, lanes])
            else:
                for n in range(SIDE):
                    put(full[half].at[n, :, rows, :], copy_out[name].at[:, n, :, lanes])
            put(new_rows[half].at[rows, :], new_out[name].at[:, lanes])
            put(state_rows[half].at[rows, :], state_out[name].at[:, lanes])
    put(full_down, copy_down)
    put(full_mixed, copy_mixed)
    put(new_down_in, new_down)
    put(state_down_in, state_down)
    put(new_mixed_in, new_mixed)
    put(state_mixed_in, state_mixed)
    for source, target in zip(norms_in, norms_out):
        put(source, target)
    for copy in copies:
        copy.wait()


PLACE_COPIES = 2 + 4 + 6 * 2 + 4 + 4 + 2 * 7 + 3


def in_hbm(arrays):
    return [pltpu.with_memory_space_constraint(a, pltpu.HBM) for a in arrays]


def body(*arrays):
    arrays = [a.T if a.ndim == 2 and a.shape[1] == ROWS else a for a in arrays]
    grads, weights, moments = arrays[:7], arrays[7:14], arrays[14:]
    shapes = [w.shape for w in weights[:6]]
    half = jax.ShapeDtypeStruct((SIDE, SIDE, HALF_ROWS, LANES), BF16)
    rows = jax.ShapeDtypeStruct((HALF_ROWS, LANES), F32)
    down, mixed = jax.ShapeDtypeStruct(shapes[1], F32), jax.ShapeDtypeStruct(shapes[5], F32)
    held = (
        half,
        half,
        jax.ShapeDtypeStruct(grads[1].shape[1:], BF16),
        jax.ShapeDtypeStruct(grads[5].shape[1:], BF16),
        rows,
        rows,
        rows,
        rows,
        down,
        down,
        mixed,
        mixed,
        jax.ShapeDtypeStruct((8 * LANES,), BF16),
        jax.ShapeDtypeStruct((1, LANES // 2), F32),
        jax.ShapeDtypeStruct((1, LANES // 2), F32),
    )
    dma = pltpu.SemaphoreType.DMA
    remote = count_remote()
    vmem = pl.BlockSpec(memory_space=pltpu.VMEM)
    anywhere = pl.BlockSpec(memory_space=pltpu.HBM)
    half_scratch = pltpu.VMEM((SIDE, SIDE, HALF_ROWS, LANES), BF16)
    part_scratch = pltpu.VMEM((SIDE, HALF_ROWS, LANES), BF16)
    from_1 = pltpu.VMEM((3, 2, SIDE, HALF_ROWS // 2, LANES), BF16)
    from_2 = pltpu.VMEM((3, HALF_ROWS, LANES), BF16)
    own = [pltpu.VMEM(s, F32) for s in shapes]
    own_packed = pltpu.VMEM((HALF_ROWS, LANES), F32)
    small = pltpu.VMEM((1, LANES // 2), F32)
    results = pl.pallas_call(
        exchange_kernel,
        out_shape=held,
        in_specs=[anywhere] * 21,
        out_specs=[vmem] * len(held),
        scratch_shapes=[
            pltpu.VMEM((7, SIDE * SIDE * ROWS, LANES), F32),
            pltpu.VMEM((5, LANES, SIDE * SIDE * ROWS), F32),
            half_scratch,
            half_scratch,
            part_scratch,
            part_scratch,
            from_1,
            from_1,
            from_2,
            from_2,
            *own,
            *own,
            own_packed,
            own_packed,
            own_packed,
            own_packed,
            pltpu.VMEM((1, 8 * LANES), F32),
            small,
            small,
            pltpu.VMEM((9, 16, LANES), F32),
            dma((27,)),
            dma((remote,)),
            dma((remote,)),
        ],
        compiler_params=pltpu.CompilerParams(
            collective_id=0, has_side_effects=True, vmem_limit_bytes=32 * 1024 * 1024
        ),
        name="exchange",
    )(
        *in_hbm(grads),
        *in_hbm(weights[:6]),
        *in_hbm([weights[6].reshape(1, -1)]),
        *in_hbm(moments[:6]),
        *in_hbm([moments[6].reshape(1, -1)]),
    )
    row_shapes = [shapes[NAMES.index(n)] for n in ROW_CUT]
    tall = [jax.ShapeDtypeStruct((SIDE, SIDE, *s), BF16) for s in row_shapes]
    own_rows = [jax.ShapeDtypeStruct(s, F32) for s in row_shapes]
    placed = pl.pallas_call(
        place_kernel,
        out_shape=(*tall, held[2], held[3], *own_rows, down, mixed, *own_rows, down, mixed, *held[12:]),
        in_specs=[vmem] * 15,
        out_specs=[anywhere] * 21,
        scratch_shapes=[dma((PLACE_COPIES,))],
        compiler_params=pltpu.CompilerParams(vmem_limit_bytes=16 * 1024 * 1024),
        name="place",
    )(*results)
    outs = []
    for k, last in zip((0, 6, 12), placed[18:]):
        up, query, key, value, down_, mixed_ = placed[k : k + 6]
        group = [up, down_, query, key, value, mixed_]
        if k == 0:
            group = [g.reshape(-1, g.shape[-1]) for g in group]
        else:
            group[1], group[5] = group[1].T, group[5].T
        outs += [*group, last.reshape(-1)]
    return tuple(outs)


def solution(mesh):
    cut_rows, cut_columns = P("batch", "cols"), P("cols", "batch")
    own = (cut_rows, cut_columns, cut_rows, cut_rows, cut_rows, cut_columns, P("batch"))
    grad_rows, grad_columns = P("batch", None, "cols"), P("batch", "cols", None)
    grads = (grad_rows, grad_columns, grad_rows, grad_rows, grad_rows, grad_columns, P("batch", None))
    whole_rows, whole_columns = P(None, "cols"), P("cols", None)
    copies = (whole_rows, whole_columns, whole_rows, whole_rows, whole_rows, whole_columns, P())
    return jax.shard_map(
        body, mesh=mesh, in_specs=(*grads, *own, *own), out_specs=(*copies, *own, *own), check_vma=False
    )
```

```python
import jax
import jax.numpy as jnp
from jax import lax
from jax.experimental import pallas as pl
from jax.experimental.pallas import tpu as pltpu
from jax.sharding import PartitionSpec as P

learn_rate = 0.1
hold_rate = 0.7

SIDE = 4
LANES = 128
ROWS = 64
NAMES = ("up", "down", "query", "key", "value", "mixed")
ROW_CUT = ("up", "query", "key", "value")

PIECES = (
    (("up", 0), ("up", 1), ("up", 2), ("up", 3), ("query", 0), ("key", 0)),
    (("value", 0), ("mixed", 0), ("down", 0), ("down", 1), ("down", 2), ("down", 3)),
)
SEGMENTS = (2, 3, 1)
HALF_ROWS = ROWS * 6
AXES = (("y", "x"), ("x", "y"))
AWAY = (1, -1, 2)
F32, BF16 = jnp.float32, jnp.bfloat16


def low_lanes(shape):
    return lax.broadcasted_iota(jnp.int32, shape, len(shape) - 1) < LANES // 2


def swap_sides(value):
    return pltpu.roll(value, LANES // 2, len(value.shape) - 1)


def interleave(first, second):
    low = low_lanes(first.shape)
    return jnp.where(low, first, swap_sides(second)), jnp.where(low, swap_sides(first), second)


def segment_spans():
    spans, at = [], 0
    for count in SEGMENTS:
        spans.append((at, count))
        at += count
    return spans


SENT_GROUPS = 9
ARRIVALS = 6


def exchange_kernel(*refs):
    refs = list(refs)

    def take(count):
        got, refs[:] = refs[:count], refs[count:]
        return got

    grad = dict(zip(NAMES, take(6)))
    (grad_norm,) = take(1)
    weight = dict(zip(NAMES, take(6)))
    (weight_norm,) = take(1)
    moment = dict(zip(NAMES, take(6)))
    (moment_norm,) = take(1)
    full = take(2)
    full_down, full_mixed = take(2)
    new_rows, state_rows = take(2), take(2)
    new_down, state_down, new_mixed, state_mixed = take(4)
    copy_norm, new_norm, state_norm = take(3)
    landed = take(2)
    packed, part = take(2), take(2)
    from_1, from_2 = take(2), take(2)
    weight_in = dict(zip(NAMES, take(6)))
    moment_in = dict(zip(NAMES, take(6)))
    weight_packed, moment_packed = take(2), take(2)
    norm_grad_in, norm_weight_in, norm_moment_in, norm_tiles = take(4)
    load_sem, send_sem, recv_sem = take(3)
    assert not refs

    me = lax.axis_index("batch")
    here = {"y": lax.div(me, SIDE), "x": lax.rem(me, SIDE)}
    step = {a: {d: lax.rem(here[a] + d + SIDE, SIDE) for d in AWAY} for a in ("y", "x")}

    def device(axis, d):
        at = dict(here)
        at[axis] = step[axis][d]
        return {"batch": at["y"] * SIDE + at["x"]}


    def load(group, source, target):
        pltpu.make_async_copy(source, target, load_sem.at[group]).start()

    def loaded(group, size_of):
        pltpu.make_async_copy(size_of, size_of, load_sem.at[group]).wait()

    own_loads = 2 * len(SEGMENTS)
    norm_loads = ((grad_norm, norm_grad_in), (weight_norm, norm_weight_in), (moment_norm, norm_moment_in))

    def load_segment(half, s):
        at, count = segment_spans()[s]
        for k in range(at, at + count):
            name, part_no = PIECES[half][k]
            lanes = pl.ds(part_no * LANES, LANES)
            if name in ROW_CUT:
                load(half * len(SEGMENTS) + s, grad[name].at[0, :, lanes], landed[0].at[slot_of(half, k)])
            else:
                load(half * len(SEGMENTS) + s, grad[name].at[0, lanes, :], landed[1].at[slot_of(half, k)])

    def load_own():
        for n, (source, target) in enumerate(norm_loads):
            load(own_loads + 1 + n, source, target)
        for name in NAMES:
            load(own_loads, weight[name], weight_in[name])
            load(own_loads, moment[name], moment_in[name])

    for half in (0, 1):
        load_segment(half, 0)
    barrier = pltpu.get_barrier_semaphore()
    for axis in ("y", "x"):
        for d in AWAY:
            pl.semaphore_signal(barrier, inc=1, device_id=device(axis, d), device_id_type=pl.DeviceIdType.MESH)

    def pack_piece(half, k):
        name, part_no = PIECES[half][k]
        rows = pl.ds(k * ROWS, ROWS)
        slot = slot_of(half, k)

        def put(b, value):
            y, x = divmod(b, SIDE)
            at = (y, x) if AXES[half][0] == "y" else (x, y)
            packed[half][at[0], at[1], rows, :] = value.astype(BF16)

        if name in ROW_CUT:
            for b in range(SIDE * SIDE):
                put(b, landed[0][slot, b * ROWS : (b + 1) * ROWS, :])
        else:
            for m in range(SIDE * SIDE // 2):
                lanes = slice(m * LANES, (m + 1) * LANES)
                pair = interleave(landed[1][slot, :ROWS, lanes], landed[1][slot, ROWS:, lanes])
                put(2 * m, pair[0])
                put(2 * m + 1, pair[1])

    def pack_own():
        loaded(own_loads, landed[0].at[0:3, 0 : SIDE * SIDE * ROWS // 2, :])
        for half in (0, 1):
            for k, (name, part_no) in enumerate(PIECES[half]):
                rows = pl.ds(k * ROWS, ROWS)
                for source, target in ((weight_in[name], weight_packed[half]), (moment_in[name], moment_packed[half])):
                    if name in ROW_CUT:
                        target[rows, :] = source[:, part_no * LANES : (part_no + 1) * LANES]
                    else:
                        turned = source[:, part_no * LANES : (part_no + 1) * LANES].T
                        target[rows, :] = jnp.concatenate([turned[:ROWS, :], turned[ROWS:, :]], axis=1)

    def remote(source, target, axis, d, group, slot):
        return pltpu.make_async_remote_copy(
            src_ref=source,
            dst_ref=target,
            send_sem=send_sem.at[group],
            recv_sem=recv_sem.at[slot],
            device_id=device(axis, d),
            device_id_type=pl.DeviceIdType.MESH,
        )

    def slot_at(half, s, kind):
        return (half * len(SEGMENTS) + s) * ARRIVALS + kind

    norm_slots = {"y": slot_at(2, 0, 0), "x": slot_at(2, 0, 1)}

    def arrived(slot, size_of):
        remote(size_of, size_of, "y", 1, 0, slot).wait_recv()

    def all_sent(group, size_of):
        remote(size_of, size_of, "y", 1, group, 0).wait_send()

    def spans(s):
        at, count = segment_spans()[s]
        rows, side = at * ROWS, count * ROWS // 2
        return (pl.ds(rows, side), pl.ds(rows + side, side), pl.ds(rows // 2, side), pl.ds(rows, 2 * side))

    def first_send(half, s):
        axis = AXES[half][0]
        low, high, place, _ = spans(s)
        data, land = packed[half], from_1[half]
        group, near, far = half * 4, slot_at(half, s, 0), slot_at(half, s, 1)
        for source, rows, kind, side, d, slot in (
            (2, low, 0, 0, 1, near),
            (2, high, 0, 1, -1, near),
            (1, high, 1, 0, 1, far),
            (-1, low, 1, 1, -1, far),
        ):
            remote(data.at[step[axis][source], :, rows, :], land.at[kind, side, :, place, :], axis, d, group, slot).start()

    def first_forward(half, s):
        axis = AXES[half][0]
        low, high, place, _ = spans(s)
        data, land = packed[half], from_1[half]
        arrived(slot_at(half, s, 0), land.at[0, :, :, place, :])
        for side, d, rows in ((0, 1, low), (1, -1, high)):
            to = step[axis][d]
            total = data[to, :, rows, :].astype(F32) + land[0, side, :, place, :].astype(F32)
            data[to, :, rows, :] = total.astype(BF16)
            target = land.at[2, side, :, place, :]
            remote(data.at[to, :, rows, :], target, axis, d, half * 4, slot_at(half, s, 1)).start()

    def second_send(half, s):
        low, high, place, whole = spans(s)
        data, land = packed[half], from_1[half]
        arrived(slot_at(half, s, 1), land.at[1:3, :, :, place, :])
        mine = here[AXES[half][0]]
        for rows, first, second in ((low, 2, 1), (high, 1, 2)):
            total = data[mine, :, rows, :].astype(F32)
            total += land[first, 0, :, place, :].astype(F32)
            total += land[second, 1, :, place, :].astype(F32)
            part[half][:, rows, :] = total.astype(BF16)
        axis = AXES[half][1]
        for n, d in ((2, 2), (0, 1), (1, -1)):
            source, target = part[half].at[step[axis][d], whole, :], from_2[half].at[n, whole, :]
            remote(source, target, axis, d, half * 4 + 1, slot_at(half, s, 2)).start()

    mean_rate = float(SIDE * SIDE) ** -0.5

    def update(half, s):
        first, second = AXES[half]
        whole = spans(s)[3]
        arrived(slot_at(half, s, 2), from_2[half].at[:, whole, :])
        total = part[half][here[second], whole, :].astype(F32)
        for n in range(3):
            total += from_2[half][n, whole, :].astype(F32)
        state = hold_rate * moment_packed[half][whole, :] + total * mean_rate
        new = weight_packed[half][whole, :] - learn_rate * state
        state_rows[half][whole, :] = state
        new_rows[half][whole, :] = new
        full[half][here[first], here[second], whole, :] = new.astype(BF16)
        own = full[half].at[here[first], here[second], whole, :]
        for d in (2, 1, -1):
            remote(own, own, second, d, half * 4 + 2, slot_at(half, s, 3)).start()

    def turn_own(half, s):
        at, count = segment_spans()[s]
        for k in range(at, at + count):
            name, part_no = PIECES[half][k]
            if name in ROW_CUT:
                continue
            rows = pl.ds(k * ROWS, ROWS)
            targets = (new_down, state_down) if name == "down" else (new_mixed, state_mixed)
            for source, target in zip((new_rows[half], state_rows[half]), targets):
                turned = source[rows, :].T
                target[:, part_no * LANES : (part_no + 1) * LANES] = jnp.concatenate([turned[:ROWS, :], turned[ROWS:, :]], axis=1)

    def share(half, s):
        whole = spans(s)[3]
        arrived(slot_at(half, s, 3), full[half].at[0, 0:3, whole, :])
        first = AXES[half][0]
        block = full[half].at[here[first], :, whole, :]
        for d in (1, -1):
            remote(block, block, first, d, half * 4 + 3, slot_at(half, s, 4)).start()
        turn_own(half, s)

    def share_forward(half, s):
        first = AXES[half][0]
        low, high, _, whole = spans(s)
        arrived(slot_at(half, s, 4), full[half].at[0:2, :, whole, :])
        for d, rows in ((1, low), (-1, high)):
            block = full[half].at[step[first][-d], :, rows, :]
            remote(block, block, first, d, half * 4 + 3, slot_at(half, s, 5)).start()

    def unpack(half, s):
        at, count = segment_spans()[s]
        for k in range(at, at + count):
            name, part_no = PIECES[half][k]
            if name in ROW_CUT:
                continue
            target = full_down if name == "down" else full_mixed
            rows = pl.ds(k * ROWS, ROWS)
            for m in range(SIDE * SIDE // 2):
                pair = []
                for b in (2 * m, 2 * m + 1):
                    y, x = divmod(b, SIDE)
                    at_ = (y, x) if AXES[half][0] == "y" else (x, y)
                    pair.append(full[half][at_[0], at_[1], rows, :].astype(F32))
                top, bottom = interleave(*pair)
                lanes = slice(m * LANES, (m + 1) * LANES)
                target[part_no * LANES : part_no * LANES + ROWS, lanes] = top.astype(BF16)
                target[part_no * LANES + ROWS : (part_no + 1) * LANES, lanes] = bottom.astype(BF16)

    def norm_start():
        for n, (_, target) in enumerate(norm_loads):
            loaded(own_loads + 1 + n, target)
        for k in range(8):
            norm_tiles[0, k : k + 1, :] = norm_grad_in[0:1, k * LANES : (k + 1) * LANES]
        base = norm_weight_in[...] - learn_rate * (hold_rate * norm_moment_in[...])
        base = jnp.broadcast_to(jnp.concatenate([base, base], axis=1), (8, LANES))
        row = lax.broadcasted_iota(jnp.int32, (8, LANES), 0)
        owner = 2 * row + jnp.where(low_lanes((8, LANES)), 0, 1)
        norm_tiles[0, 8:16, :] = jnp.where(owner == me, base, 0.0)
        norm_send("y", 0)

    def norm_send(axis, at):
        for n, d in enumerate(AWAY):
            remote(norm_tiles.at[at], norm_tiles.at[at + 1 + n], axis, d, 8, norm_slots[axis]).start()

    def norm_total(axis, at):
        arrived(norm_slots[axis], norm_tiles.at[at + 1 : at + 4])
        return (norm_tiles[at] + norm_tiles[at + 1]) + (norm_tiles[at + 2] + norm_tiles[at + 3])

    def norm_middle():
        norm_tiles[4] = norm_total("y", 0)
        norm_send("x", 4)

    def norm_end():
        total = norm_total("x", 4)
        mean = total[0:8, :] * mean_rate
        norm_tiles[8, 0:8, :] = mean
        new = (total[8:16, :] - learn_rate * mean).astype(BF16)
        for k in range(8):
            copy_norm[k * LANES : (k + 1) * LANES] = new[k, :]
        own = norm_tiles[8, pl.ds(lax.div(me, 2), 1), :]
        own = jnp.where(lax.rem(me, 2) == 1, swap_sides(own), own)[:, : LANES // 2]
        state = hold_rate * norm_moment_in[...] + own
        state_norm[...] = state
        new_norm[...] = norm_weight_in[...] - learn_rate * state

    def begin(half, s):
        at, count = segment_spans()[s]
        loaded(half * len(SEGMENTS) + s, landed[0].at[0:count])
        for k in range(at, at + count):
            pack_piece(half, k)
        if half == 0 and s == 0:
            pl.semaphore_wait(barrier, 2 * len(AWAY))
        first_send(half, s)
        if s + 1 < len(SEGMENTS):
            load_segment(half, s + 1)
        elif half == 1:
            load_own()

    def finish(half, s):
        arrived(slot_at(half, s, 5), full[half].at[0, :, spans(s)[3], :])
        unpack(half, s)

    stages = (begin, first_forward, second_send, update, share, share_forward, finish)
    after = {0: (norm_start,), 1: (norm_middle, pack_own), 2: (norm_end,)}
    for n, stage in enumerate(stages):
        for s in range(len(SEGMENTS)):
            for half in (0, 1):
                stage(half, s)
        for extra in after.get(n, ()):
            extra()
    for half in (0, 1):
        for n, size_of in enumerate((from_1[half], from_2[half], from_2[half], from_1[half])):
            all_sent(half * 4 + n, size_of)
    all_sent(8, norm_tiles.at[0:6])


def slot_of(half, k):
    order = [p for h in (0, 1) for p in PIECES[h]]
    this = PIECES[half][k]
    kind = this[0] in ROW_CUT
    return [p for p in order if (p[0] in ROW_CUT) == kind].index(this)


def place_kernel(*refs):
    refs = list(refs)

    def take(count):
        got, refs[:] = refs[:count], refs[count:]
        return got

    full = take(2)
    full_down, full_mixed = take(2)
    new_rows, state_rows = take(2), take(2)
    new_down_in, state_down_in, new_mixed_in, state_mixed_in = take(4)
    norms_in = take(3)
    copy_out = dict(zip(ROW_CUT, take(4)))
    copy_down, copy_mixed = take(2)
    new_out = dict(zip(ROW_CUT, take(4)))
    new_down, new_mixed = take(2)
    state_out = dict(zip(ROW_CUT, take(4)))
    state_down, state_mixed = take(2)
    norms_out = take(3)
    (sem,) = take(1)
    assert not refs

    def put(source, target, group):
        pltpu.make_async_copy(source, target, sem.at[group]).start()

    for half in (0, 1):
        for k, (name, part_no) in enumerate(PIECES[half]):
            if name not in ROW_CUT:
                continue
            rows, lanes = pl.ds(k * ROWS, ROWS), pl.ds(part_no * LANES, LANES)
            if AXES[half][0] == "y":
                put(full[half].at[:, :, rows, :], copy_out[name].at[:, :, :, lanes], 0)
            else:
                for n in range(SIDE):
                    put(full[half].at[n, :, rows, :], copy_out[name].at[:, n, :, lanes], 1)
            put(new_rows[half].at[rows, :], new_out[name].at[:, lanes], 2)
            put(state_rows[half].at[rows, :], state_out[name].at[:, lanes], 2)
    put(full_down, copy_down, 1)
    put(full_mixed, copy_mixed, 1)
    put(new_down_in, new_down, 2)
    put(state_down_in, state_down, 2)
    put(new_mixed_in, new_mixed, 2)
    put(state_mixed_in, state_mixed, 2)
    for n, (source, target) in enumerate(zip(norms_in, norms_out)):
        put(source, target, 3 + n)
    for group, size_of in enumerate((full[0], full[1], full[0].at[0:2], *norms_in)):
        pltpu.make_async_copy(size_of, size_of, sem.at[group]).wait()


def in_hbm(arrays):
    return [pltpu.with_memory_space_constraint(a, pltpu.HBM) for a in arrays]


def body(*arrays):
    arrays = [a.T if a.ndim == 2 and a.shape[1] == ROWS else a for a in arrays]
    grads, weights, moments = arrays[:7], arrays[7:14], arrays[14:]
    shapes = [w.shape for w in weights[:6]]
    half = jax.ShapeDtypeStruct((SIDE, SIDE, HALF_ROWS, LANES), BF16)
    rows = jax.ShapeDtypeStruct((HALF_ROWS, LANES), F32)
    down, mixed = jax.ShapeDtypeStruct(shapes[1], F32), jax.ShapeDtypeStruct(shapes[5], F32)
    held = (
        half,
        half,
        jax.ShapeDtypeStruct(grads[1].shape[1:], BF16),
        jax.ShapeDtypeStruct(grads[5].shape[1:], BF16),
        rows,
        rows,
        rows,
        rows,
        down,
        down,
        mixed,
        mixed,
        jax.ShapeDtypeStruct((8 * LANES,), BF16),
        jax.ShapeDtypeStruct((1, LANES // 2), F32),
        jax.ShapeDtypeStruct((1, LANES // 2), F32),
    )
    dma = pltpu.SemaphoreType.DMA
    remote = 2 * len(SEGMENTS) * ARRIVALS + 2
    vmem = pl.BlockSpec(memory_space=pltpu.VMEM)
    anywhere = pl.BlockSpec(memory_space=pltpu.HBM)
    half_scratch = pltpu.VMEM((SIDE, SIDE, HALF_ROWS, LANES), BF16)
    part_scratch = pltpu.VMEM((SIDE, HALF_ROWS, LANES), BF16)
    from_1 = pltpu.VMEM((3, 2, SIDE, HALF_ROWS // 2, LANES), BF16)
    from_2 = pltpu.VMEM((3, HALF_ROWS, LANES), BF16)
    own = [pltpu.VMEM(s, F32) for s in shapes]
    own_packed = pltpu.VMEM((HALF_ROWS, LANES), F32)
    small = pltpu.VMEM((1, LANES // 2), F32)
    results = pl.pallas_call(
        exchange_kernel,
        out_shape=held,
        in_specs=[anywhere] * 21,
        out_specs=[vmem] * len(held),
        scratch_shapes=[
            pltpu.VMEM((7, SIDE * SIDE * ROWS, LANES), F32),
            pltpu.VMEM((5, LANES, SIDE * SIDE * ROWS), F32),
            half_scratch,
            half_scratch,
            part_scratch,
            part_scratch,
            from_1,
            from_1,
            from_2,
            from_2,
            *own,
            *own,
            own_packed,
            own_packed,
            own_packed,
            own_packed,
            pltpu.VMEM((1, 8 * LANES), F32),
            small,
            small,
            pltpu.VMEM((9, 16, LANES), F32),
            dma((2 * len(SEGMENTS) + 4,)),
            dma((SENT_GROUPS,)),
            dma((remote,)),
        ],
        compiler_params=pltpu.CompilerParams(
            collective_id=0, has_side_effects=True, vmem_limit_bytes=32 * 1024 * 1024
        ),
        name="exchange",
    )(
        *in_hbm(grads),
        *in_hbm(weights[:6]),
        *in_hbm([weights[6].reshape(1, -1)]),
        *in_hbm(moments[:6]),
        *in_hbm([moments[6].reshape(1, -1)]),
    )
    row_shapes = [shapes[NAMES.index(n)] for n in ROW_CUT]
    tall = [jax.ShapeDtypeStruct((SIDE, SIDE, *s), BF16) for s in row_shapes]
    own_rows = [jax.ShapeDtypeStruct(s, F32) for s in row_shapes]
    placed = pl.pallas_call(
        place_kernel,
        out_shape=(*tall, held[2], held[3], *own_rows, down, mixed, *own_rows, down, mixed, *held[12:]),
        in_specs=[vmem] * 15,
        out_specs=[anywhere] * 21,
        scratch_shapes=[dma((6,))],
        compiler_params=pltpu.CompilerParams(vmem_limit_bytes=16 * 1024 * 1024),
        name="place",
    )(*results)
    outs = []
    for k, last in zip((0, 6, 12), placed[18:]):
        up, query, key, value, down_, mixed_ = placed[k : k + 6]
        group = [up, down_, query, key, value, mixed_]
        if k == 0:
            group = [g.reshape(-1, g.shape[-1]) for g in group]
        else:
            group[1], group[5] = group[1].T, group[5].T
        outs += [*group, last.reshape(-1)]
    return tuple(outs)


def solution(mesh):
    cut_rows, cut_columns = P("batch", "cols"), P("cols", "batch")
    own = (cut_rows, cut_columns, cut_rows, cut_rows, cut_rows, cut_columns, P("batch"))
    grad_rows, grad_columns = P("batch", None, "cols"), P("batch", "cols", None)
    grads = (grad_rows, grad_columns, grad_rows, grad_rows, grad_rows, grad_columns, P("batch", None))
    whole_rows, whole_columns = P(None, "cols"), P("cols", None)
    copies = (whole_rows, whole_columns, whole_rows, whole_rows, whole_rows, whole_columns, P())
    return jax.shard_map(
        body, mesh=mesh, in_specs=(*grads, *own, *own), out_specs=(*copies, *own, *own), check_vma=False
    )
```

```python
import jax
import jax.numpy as jnp
from jax import lax
from jax.experimental import pallas as pl
from jax.experimental.pallas import tpu as pltpu
from jax.sharding import PartitionSpec as P

learn_rate = 0.1
hold_rate = 0.7

SIDE = 4
LANES = 128
ROWS = 64
NAMES = ("up", "down", "query", "key", "value", "mixed")
ROW_CUT = ("up", "query", "key", "value")

PIECES = (
    (("up", 0), ("up", 1), ("up", 2), ("up", 3), ("query", 0), ("key", 0)),
    (("value", 0), ("mixed", 0), ("down", 0), ("down", 1), ("down", 2), ("down", 3)),
)
SEGMENTS = (2, 3, 1)
HALF_ROWS = ROWS * 6
REDUCE = ("B0", "B1", "B2", "N", "F0", "F1", "F2", "M", "O", "T0", "T1", "T2", "X")
GATHER_FAR = ("U0", "U1", "U2", "S0", "S1", "S2", "G0", "G1", "G2", "E0", "E1", "E2")
GATHER_NEAR = ("U0", "U1", "U2", "S0", "S1", "S2", "L0", "L1", "L2", "G0", "G1", "G2", "E0", "E1", "E2")
AXES = (("y", "x"), ("x", "y"))
AWAY = (1, -1, 2)
F32, BF16 = jnp.float32, jnp.bfloat16


def low_lanes(shape):
    return lax.broadcasted_iota(jnp.int32, shape, len(shape) - 1) < LANES // 2


def swap_sides(value):
    return pltpu.roll(value, LANES // 2, len(value.shape) - 1)


def interleave(first, second):
    low = low_lanes(first.shape)
    return jnp.where(low, first, swap_sides(second)), jnp.where(low, swap_sides(first), second)


def segment_spans():
    spans, at = [], 0
    for count in SEGMENTS:
        spans.append((at, count))
        at += count
    return spans


SENT_GROUPS = 9
ARRIVALS = 7


def exchange_kernel(*refs):
    refs = list(refs)

    def take(count):
        got, refs[:] = refs[:count], refs[count:]
        return got

    grad = dict(zip(NAMES, take(6)))
    (grad_norm,) = take(1)
    weight = dict(zip(NAMES, take(6)))
    (weight_norm,) = take(1)
    moment = dict(zip(NAMES, take(6)))
    (moment_norm,) = take(1)
    full = take(2)
    full_down, full_mixed = take(2)
    new_rows, state_rows = take(2), take(2)
    new_down, state_down, new_mixed, state_mixed = take(4)
    copy_norm, new_norm, state_norm = take(3)
    landed = take(2)
    packed, part = take(2), take(2)
    from_1, from_2 = take(2), take(2)
    weight_in = dict(zip(NAMES, take(6)))
    moment_in = dict(zip(NAMES, take(6)))
    weight_packed, moment_packed = take(2), take(2)
    norm_grad_in, norm_weight_in, norm_moment_in, norm_tiles = take(4)
    load_sem, send_sem, recv_sem = take(3)
    assert not refs

    me = lax.axis_index("batch")
    here = {"y": lax.div(me, SIDE), "x": lax.rem(me, SIDE)}
    step = {a: {d: lax.rem(here[a] + d + SIDE, SIDE) for d in AWAY} for a in ("y", "x")}

    def device(axis, d):
        at = dict(here)
        at[axis] = step[axis][d]
        return {"batch": at["y"] * SIDE + at["x"]}


    def load(group, source, target):
        pltpu.make_async_copy(source, target, load_sem.at[group]).start()

    def loaded(group, size_of):
        pltpu.make_async_copy(size_of, size_of, load_sem.at[group]).wait()

    own_loads = 2 * len(SEGMENTS)
    norm_loads = ((grad_norm, norm_grad_in), (weight_norm, norm_weight_in), (moment_norm, norm_moment_in))

    def load_segment(half, s):
        at, count = segment_spans()[s]
        for k in range(at, at + count):
            name, part_no = PIECES[half][k]
            lanes = pl.ds(part_no * LANES, LANES)
            if name in ROW_CUT:
                load(half * len(SEGMENTS) + s, grad[name].at[0, :, lanes], landed[0].at[slot_of(half, k)])
            else:
                load(half * len(SEGMENTS) + s, grad[name].at[0, lanes, :], landed[1].at[slot_of(half, k)])

    def load_own():
        for n, (source, target) in enumerate(norm_loads):
            load(own_loads + 1 + n, source, target)
        for name in NAMES:
            load(own_loads, weight[name], weight_in[name])
            load(own_loads, moment[name], moment_in[name])

    for half in (0, 1):
        load_segment(half, 0)
    barrier = pltpu.get_barrier_semaphore()
    for axis in ("y", "x"):
        for d in AWAY:
            pl.semaphore_signal(barrier, inc=1, device_id=device(axis, d), device_id_type=pl.DeviceIdType.MESH)

    def pack_piece(half, k):
        name, part_no = PIECES[half][k]
        rows = pl.ds(k * ROWS, ROWS)
        slot = slot_of(half, k)

        def put(b, value):
            y, x = divmod(b, SIDE)
            at = (y, x) if AXES[half][0] == "y" else (x, y)
            packed[half][at[0], at[1], rows, :] = value.astype(BF16)

        if name in ROW_CUT:
            for b in range(SIDE * SIDE):
                put(b, landed[0][slot, b * ROWS : (b + 1) * ROWS, :])
        else:
            for m in range(SIDE * SIDE // 2):
                lanes = slice(m * LANES, (m + 1) * LANES)
                pair = interleave(landed[1][slot, :ROWS, lanes], landed[1][slot, ROWS:, lanes])
                put(2 * m, pair[0])
                put(2 * m + 1, pair[1])

    def pack_own():
        loaded(own_loads, landed[0].at[0:3, 0 : SIDE * SIDE * ROWS // 2, :])
        for half in (0, 1):
            for k, (name, part_no) in enumerate(PIECES[half]):
                rows = pl.ds(k * ROWS, ROWS)
                for source, target in ((weight_in[name], weight_packed[half]), (moment_in[name], moment_packed[half])):
                    if name in ROW_CUT:
                        target[rows, :] = source[:, part_no * LANES : (part_no + 1) * LANES]
                    else:
                        turned = source[:, part_no * LANES : (part_no + 1) * LANES].T
                        target[rows, :] = jnp.concatenate([turned[:ROWS, :], turned[ROWS:, :]], axis=1)

    def remote(source, target, axis, d, group, slot):
        return pltpu.make_async_remote_copy(
            src_ref=source,
            dst_ref=target,
            send_sem=send_sem.at[group],
            recv_sem=recv_sem.at[slot],
            device_id=device(axis, d),
            device_id_type=pl.DeviceIdType.MESH,
        )

    def slot_at(half, s, kind):
        return (half * len(SEGMENTS) + s) * ARRIVALS + kind

    norm_slots = {"y": slot_at(2, 0, 0), "x": slot_at(2, 0, 1)}

    def arrived(slot, size_of):
        remote(size_of, size_of, "y", 1, 0, slot).wait_recv()

    def all_sent(group, size_of):
        remote(size_of, size_of, "y", 1, group, 0).wait_send()

    def spans(s):
        at, count = segment_spans()[s]
        rows, side = at * ROWS, count * ROWS // 2
        return (pl.ds(rows, side), pl.ds(rows + side, side), pl.ds(rows // 2, side), pl.ds(rows, 2 * side))

    def first_send(half, s):
        axis = AXES[half][0]
        low, high, place, _ = spans(s)
        data, land = packed[half], from_1[half]
        group, near, far = half * 4, slot_at(half, s, 0), slot_at(half, s, 1)
        for source, rows, kind, side, d, slot in (
            (2, low, 0, 0, 1, near),
            (2, high, 0, 1, -1, near),
            (1, high, 1, 0, 1, far),
            (-1, low, 1, 1, -1, far),
        ):
            remote(data.at[step[axis][source], :, rows, :], land.at[kind, side, :, place, :], axis, d, group, slot).start()

    def first_forward(half, s):
        axis = AXES[half][0]
        low, high, place, _ = spans(s)
        data, land = packed[half], from_1[half]
        arrived(slot_at(half, s, 0), land.at[0, :, :, place, :])
        for side, d, rows in ((0, 1, low), (1, -1, high)):
            to = step[axis][d]
            total = data[to, :, rows, :].astype(F32) + land[0, side, :, place, :].astype(F32)
            data[to, :, rows, :] = total.astype(BF16)
            target = land.at[2, side, :, place, :]
            remote(data.at[to, :, rows, :], target, axis, d, half * 4, slot_at(half, s, 1)).start()

    def second_send(half, s):
        low, high, place, whole = spans(s)
        data, land = packed[half], from_1[half]
        arrived(slot_at(half, s, 1), land.at[1:3, :, :, place, :])
        mine = here[AXES[half][0]]
        for rows, first, second in ((low, 2, 1), (high, 1, 2)):
            total = data[mine, :, rows, :].astype(F32)
            total += land[first, 0, :, place, :].astype(F32)
            total += land[second, 1, :, place, :].astype(F32)
            part[half][:, rows, :] = total.astype(BF16)
        axis = AXES[half][1]
        for n, d in ((2, 2), (0, 1), (1, -1)):
            source, target = part[half].at[step[axis][d], whole, :], from_2[half].at[n, whole, :]
            remote(source, target, axis, d, half * 4 + 1, slot_at(half, s, 2)).start()

    mean_rate = float(SIDE * SIDE) ** -0.5

    def update(half, s, far):
        first, second = AXES[half]
        whole = spans(s)[3]
        arrived(slot_at(half, s, 2), from_2[half].at[:, whole, :])
        total = part[half][here[second], whole, :].astype(F32)
        for n in range(3):
            total += from_2[half][n, whole, :].astype(F32)
        state = hold_rate * moment_packed[half][whole, :] + total * mean_rate
        new = weight_packed[half][whole, :] - learn_rate * state
        state_rows[half][whole, :] = state
        new_rows[half][whole, :] = new
        full[half][here[first], here[second], whole, :] = new.astype(BF16)
        own = full[half].at[here[first], here[second], whole, :]
        for d in (2, 1, -1) if far else (1, -1):
            remote(own, own, second, d, half * 4 + 2, slot_at(half, s, 3)).start()
        if not far:
            share_block(half, s, 0)

    def turn_own(half, s):
        at, count = segment_spans()[s]
        for k in range(at, at + count):
            name, part_no = PIECES[half][k]
            if name in ROW_CUT:
                continue
            rows = pl.ds(k * ROWS, ROWS)
            targets = (new_down, state_down) if name == "down" else (new_mixed, state_mixed)
            for source, target in zip((new_rows[half], state_rows[half]), targets):
                turned = source[rows, :].T
                target[:, part_no * LANES : (part_no + 1) * LANES] = jnp.concatenate([turned[:ROWS, :], turned[ROWS:, :]], axis=1)

    def share_block(half, s, away):
        first, second = AXES[half]
        at = step[second][away] if away else here[second]
        block = full[half].at[here[first], at, spans(s)[3], :]
        for d in (1, -1):
            remote(block, block, first, d, half * 4 + 3, slot_at(half, s, 5)).start()

    def share_all(half, s):
        first = AXES[half][0]
        whole = spans(s)[3]
        arrived(slot_at(half, s, 3), full[half].at[0, 0:3, whole, :])
        block = full[half].at[here[first], :, whole, :]
        for d in (1, -1):
            remote(block, block, first, d, half * 4 + 3, slot_at(half, s, 5)).start()
        turn_own(half, s)

    def share(half, s):
        first, second = AXES[half]
        low, high, _, whole = spans(s)
        arrived(slot_at(half, s, 3), full[half].at[0, 0:2, whole, :])
        for d, rows in ((1, low), (-1, high)):
            block = full[half].at[here[first], step[second][-d], rows, :]
            remote(block, block, second, d, half * 4 + 2, slot_at(half, s, 4)).start()
        for away in (1, -1):
            share_block(half, s, away)
        turn_own(half, s)

    def share_last(half, s):
        arrived(slot_at(half, s, 4), full[half].at[0, 0, spans(s)[3], :])
        share_block(half, s, 2)

    def share_forward(half, s):
        first = AXES[half][0]
        low, high, _, whole = spans(s)
        arrived(slot_at(half, s, 5), full[half].at[0:2, :, whole, :])
        for d, rows in ((1, low), (-1, high)):
            block = full[half].at[step[first][-d], :, rows, :]
            remote(block, block, first, d, half * 4 + 3, slot_at(half, s, 6)).start()

    def unpack(half, s):
        at, count = segment_spans()[s]
        for k in range(at, at + count):
            name, part_no = PIECES[half][k]
            if name in ROW_CUT:
                continue
            target = full_down if name == "down" else full_mixed
            rows = pl.ds(k * ROWS, ROWS)
            for m in range(SIDE * SIDE // 2):
                pair = []
                for b in (2 * m, 2 * m + 1):
                    y, x = divmod(b, SIDE)
                    at_ = (y, x) if AXES[half][0] == "y" else (x, y)
                    pair.append(full[half][at_[0], at_[1], rows, :].astype(F32))
                top, bottom = interleave(*pair)
                lanes = slice(m * LANES, (m + 1) * LANES)
                target[part_no * LANES : part_no * LANES + ROWS, lanes] = top.astype(BF16)
                target[part_no * LANES + ROWS : (part_no + 1) * LANES, lanes] = bottom.astype(BF16)

    def norm_start():
        for n, (_, target) in enumerate(norm_loads):
            loaded(own_loads + 1 + n, target)
        for k in range(8):
            norm_tiles[0, k : k + 1, :] = norm_grad_in[0:1, k * LANES : (k + 1) * LANES]
        base = norm_weight_in[...] - learn_rate * (hold_rate * norm_moment_in[...])
        base = jnp.broadcast_to(jnp.concatenate([base, base], axis=1), (8, LANES))
        row = lax.broadcasted_iota(jnp.int32, (8, LANES), 0)
        owner = 2 * row + jnp.where(low_lanes((8, LANES)), 0, 1)
        norm_tiles[0, 8:16, :] = jnp.where(owner == me, base, 0.0)
        norm_send("y", 0)

    def norm_send(axis, at):
        for n, d in enumerate(AWAY):
            remote(norm_tiles.at[at], norm_tiles.at[at + 1 + n], axis, d, 8, norm_slots[axis]).start()

    def norm_total(axis, at):
        arrived(norm_slots[axis], norm_tiles.at[at + 1 : at + 4])
        return (norm_tiles[at] + norm_tiles[at + 1]) + (norm_tiles[at + 2] + norm_tiles[at + 3])

    def norm_middle():
        norm_tiles[4] = norm_total("y", 0)
        norm_send("x", 4)

    def norm_end():
        total = norm_total("x", 4)
        mean = total[0:8, :] * mean_rate
        norm_tiles[8, 0:8, :] = mean
        new = (total[8:16, :] - learn_rate * mean).astype(BF16)
        for k in range(8):
            copy_norm[k * LANES : (k + 1) * LANES] = new[k, :]
        own = norm_tiles[8, pl.ds(lax.div(me, 2), 1), :]
        own = jnp.where(lax.rem(me, 2) == 1, swap_sides(own), own)[:, : LANES // 2]
        state = hold_rate * norm_moment_in[...] + own
        state_norm[...] = state
        new_norm[...] = norm_weight_in[...] - learn_rate * state

    def begin(half, s):
        at, count = segment_spans()[s]
        loaded(half * len(SEGMENTS) + s, landed[0].at[0:count])
        for k in range(at, at + count):
            pack_piece(half, k)
        if half == 0 and s == 0:
            pl.semaphore_wait(barrier, 2 * len(AWAY))
        first_send(half, s)
        if s + 1 < len(SEGMENTS):
            load_segment(half, s + 1)
        elif half == 1:
            load_own()

    def finish(half, s):
        arrived(slot_at(half, s, 6), full[half].at[0, :, spans(s)[3], :])
        unpack(half, s)

    def run(order, far=False):
        stages = dict(
            B=begin,
            F=first_forward,
            T=second_send,
            U=lambda half, s: update(half, s, far),
            S=share_all if far else share,
            L=share_last,
            G=share_forward,
            E=finish,
        )
        extras = dict(N=norm_start, M=norm_middle, O=pack_own, X=norm_end)
        for name in order:
            if name in extras:
                extras[name]()
            else:
                for half in (0, 1):
                    stages[name[0]](half, int(name[1]))

    run(REDUCE)
    core = lax.rem(lax.axis_index("cols"), 2)
    pl.when(core == 0)(lambda: run(GATHER_FAR, far=True))
    pl.when(core == 1)(lambda: run(GATHER_NEAR))
    for half in (0, 1):
        for n, size_of in enumerate((from_1[half], from_2[half], from_2[half], from_1[half])):
            all_sent(half * 4 + n, size_of)
    all_sent(8, norm_tiles.at[0:6])


def slot_of(half, k):
    order = [p for h in (0, 1) for p in PIECES[h]]
    this = PIECES[half][k]
    kind = this[0] in ROW_CUT
    return [p for p in order if (p[0] in ROW_CUT) == kind].index(this)


def place_kernel(*refs):
    refs = list(refs)

    def take(count):
        got, refs[:] = refs[:count], refs[count:]
        return got

    full = take(2)
    full_down, full_mixed = take(2)
    new_rows, state_rows = take(2), take(2)
    new_down_in, state_down_in, new_mixed_in, state_mixed_in = take(4)
    norms_in = take(3)
    copy_out = dict(zip(ROW_CUT, take(4)))
    copy_down, copy_mixed = take(2)
    new_out = dict(zip(ROW_CUT, take(4)))
    new_down, new_mixed = take(2)
    state_out = dict(zip(ROW_CUT, take(4)))
    state_down, state_mixed = take(2)
    norms_out = take(3)
    (sem,) = take(1)
    assert not refs

    def put(source, target, group):
        pltpu.make_async_copy(source, target, sem.at[group]).start()

    for half in (0, 1):
        for k, (name, part_no) in enumerate(PIECES[half]):
            if name not in ROW_CUT:
                continue
            rows, lanes = pl.ds(k * ROWS, ROWS), pl.ds(part_no * LANES, LANES)
            if AXES[half][0] == "y":
                put(full[half].at[:, :, rows, :], copy_out[name].at[:, :, :, lanes], 0)
            else:
                for n in range(SIDE):
                    put(full[half].at[n, :, rows, :], copy_out[name].at[:, n, :, lanes], 1)
            put(new_rows[half].at[rows, :], new_out[name].at[:, lanes], 2)
            put(state_rows[half].at[rows, :], state_out[name].at[:, lanes], 2)
    put(full_down, copy_down, 1)
    put(full_mixed, copy_mixed, 1)
    put(new_down_in, new_down, 2)
    put(state_down_in, state_down, 2)
    put(new_mixed_in, new_mixed, 2)
    put(state_mixed_in, state_mixed, 2)
    for n, (source, target) in enumerate(zip(norms_in, norms_out)):
        put(source, target, 3 + n)
    for group, size_of in enumerate((full[0], full[1], full[0].at[0:2], *norms_in)):
        pltpu.make_async_copy(size_of, size_of, sem.at[group]).wait()


def in_hbm(arrays):
    return [pltpu.with_memory_space_constraint(a, pltpu.HBM) for a in arrays]


def body(*arrays):
    arrays = [a.T if a.ndim == 2 and a.shape[1] == ROWS else a for a in arrays]
    grads, weights, moments = arrays[:7], arrays[7:14], arrays[14:]
    shapes = [w.shape for w in weights[:6]]
    half = jax.ShapeDtypeStruct((SIDE, SIDE, HALF_ROWS, LANES), BF16)
    rows = jax.ShapeDtypeStruct((HALF_ROWS, LANES), F32)
    down, mixed = jax.ShapeDtypeStruct(shapes[1], F32), jax.ShapeDtypeStruct(shapes[5], F32)
    held = (
        half,
        half,
        jax.ShapeDtypeStruct(grads[1].shape[1:], BF16),
        jax.ShapeDtypeStruct(grads[5].shape[1:], BF16),
        rows,
        rows,
        rows,
        rows,
        down,
        down,
        mixed,
        mixed,
        jax.ShapeDtypeStruct((8 * LANES,), BF16),
        jax.ShapeDtypeStruct((1, LANES // 2), F32),
        jax.ShapeDtypeStruct((1, LANES // 2), F32),
    )
    dma = pltpu.SemaphoreType.DMA
    remote = 2 * len(SEGMENTS) * ARRIVALS + 2
    vmem = pl.BlockSpec(memory_space=pltpu.VMEM)
    anywhere = pl.BlockSpec(memory_space=pltpu.HBM)
    half_scratch = pltpu.VMEM((SIDE, SIDE, HALF_ROWS, LANES), BF16)
    part_scratch = pltpu.VMEM((SIDE, HALF_ROWS, LANES), BF16)
    from_1 = pltpu.VMEM((3, 2, SIDE, HALF_ROWS // 2, LANES), BF16)
    from_2 = pltpu.VMEM((3, HALF_ROWS, LANES), BF16)
    own = [pltpu.VMEM(s, F32) for s in shapes]
    own_packed = pltpu.VMEM((HALF_ROWS, LANES), F32)
    small = pltpu.VMEM((1, LANES // 2), F32)
    results = pl.pallas_call(
        exchange_kernel,
        out_shape=held,
        in_specs=[anywhere] * 21,
        out_specs=[vmem] * len(held),
        scratch_shapes=[
            pltpu.VMEM((7, SIDE * SIDE * ROWS, LANES), F32),
            pltpu.VMEM((5, LANES, SIDE * SIDE * ROWS), F32),
            half_scratch,
            half_scratch,
            part_scratch,
            part_scratch,
            from_1,
            from_1,
            from_2,
            from_2,
            *own,
            *own,
            own_packed,
            own_packed,
            own_packed,
            own_packed,
            pltpu.VMEM((1, 8 * LANES), F32),
            small,
            small,
            pltpu.VMEM((9, 16, LANES), F32),
            dma((2 * len(SEGMENTS) + 4,)),
            dma((SENT_GROUPS,)),
            dma((remote,)),
        ],
        compiler_params=pltpu.CompilerParams(
            collective_id=0, has_side_effects=True, vmem_limit_bytes=32 * 1024 * 1024
        ),
        name="exchange",
    )(
        *in_hbm(grads),
        *in_hbm(weights[:6]),
        *in_hbm([weights[6].reshape(1, -1)]),
        *in_hbm(moments[:6]),
        *in_hbm([moments[6].reshape(1, -1)]),
    )
    row_shapes = [shapes[NAMES.index(n)] for n in ROW_CUT]
    tall = [jax.ShapeDtypeStruct((SIDE, SIDE, *s), BF16) for s in row_shapes]
    own_rows = [jax.ShapeDtypeStruct(s, F32) for s in row_shapes]
    placed = pl.pallas_call(
        place_kernel,
        out_shape=(*tall, held[2], held[3], *own_rows, down, mixed, *own_rows, down, mixed, *held[12:]),
        in_specs=[vmem] * 15,
        out_specs=[anywhere] * 21,
        scratch_shapes=[dma((6,))],
        compiler_params=pltpu.CompilerParams(vmem_limit_bytes=16 * 1024 * 1024),
        name="place",
    )(*results)
    outs = []
    for k, last in zip((0, 6, 12), placed[18:]):
        up, query, key, value, down_, mixed_ = placed[k : k + 6]
        group = [up, down_, query, key, value, mixed_]
        if k == 0:
            group = [g.reshape(-1, g.shape[-1]) for g in group]
        else:
            group[1], group[5] = group[1].T, group[5].T
        outs += [*group, last.reshape(-1)]
    return tuple(outs)


def solution(mesh):
    cut_rows, cut_columns = P("batch", "cols"), P("cols", "batch")
    own = (cut_rows, cut_columns, cut_rows, cut_rows, cut_rows, cut_columns, P("batch"))
    grad_rows, grad_columns = P("batch", None, "cols"), P("batch", "cols", None)
    grads = (grad_rows, grad_columns, grad_rows, grad_rows, grad_rows, grad_columns, P("batch", None))
    whole_rows, whole_columns = P(None, "cols"), P("cols", None)
    copies = (whole_rows, whole_columns, whole_rows, whole_rows, whole_rows, whole_columns, P())
    return jax.shard_map(
        body, mesh=mesh, in_specs=(*grads, *own, *own), out_specs=(*copies, *own, *own), check_vma=False
    )
```

```python
import jax
import jax.numpy as jnp
from jax import lax
from jax.experimental import pallas as pl
from jax.experimental.pallas import tpu as pltpu
from jax.sharding import PartitionSpec as P

learn_rate = 0.1
hold_rate = 0.7

SIDE = 4
LANES = 128
ROWS = 64
NAMES = ("up", "down", "query", "key", "value", "mixed")
ROW_CUT = ("up", "query", "key", "value")

PIECES = (
    (("up", 0), ("up", 1), ("up", 2), ("up", 3), ("query", 0), ("key", 0)),
    (("value", 0), ("mixed", 0), ("down", 0), ("down", 1), ("down", 2), ("down", 3)),
)
SEGMENTS = (2, 3, 1)
HALF_ROWS = ROWS * 6
REDUCE = ("B0", "B1", "B2", "F0", "N", "F1", "F2", "O", "T0", "T1", "M", "T2")
GATHER_FAR = ("U0", "U1", "U2", "X", "S0", "S1", "S2", "G0", "G1", "G2", "E0", "E1", "E2")
GATHER_NEAR = ("U0", "U1", "U2", "X", "S0", "S1", "S2", "L0", "L1", "L2", "G0", "G1", "G2", "E0", "E1", "E2")
AXES = (("y", "x"), ("x", "y"))
AWAY = (1, -1, 2)
F32, BF16 = jnp.float32, jnp.bfloat16


def low_lanes(shape):
    return lax.broadcasted_iota(jnp.int32, shape, len(shape) - 1) < LANES // 2


def swap_sides(value):
    return pltpu.roll(value, LANES // 2, len(value.shape) - 1)


def interleave(first, second):
    low = low_lanes(first.shape)
    return jnp.where(low, first, swap_sides(second)), jnp.where(low, swap_sides(first), second)


def segment_spans():
    spans, at = [], 0
    for count in SEGMENTS:
        spans.append((at, count))
        at += count
    return spans


SENT_GROUPS = 9
ARRIVALS = 7


def exchange_kernel(*refs):
    refs = list(refs)

    def take(count):
        got, refs[:] = refs[:count], refs[count:]
        return got

    grad = dict(zip(NAMES, take(6)))
    (grad_norm,) = take(1)
    weight = dict(zip(NAMES, take(6)))
    (weight_norm,) = take(1)
    moment = dict(zip(NAMES, take(6)))
    (moment_norm,) = take(1)
    full = take(2)
    full_down, full_mixed = take(2)
    new_rows, state_rows = take(2), take(2)
    new_down, state_down, new_mixed, state_mixed = take(4)
    copy_norm, new_norm, state_norm = take(3)
    landed = take(2)
    packed, part = take(2), take(2)
    from_1, from_2 = take(2), take(2)
    weight_in = dict(zip(NAMES, take(6)))
    moment_in = dict(zip(NAMES, take(6)))
    weight_packed, moment_packed = take(2), take(2)
    norm_grad_in, norm_weight_in, norm_moment_in, norm_tiles = take(4)
    load_sem, send_sem, recv_sem = take(3)
    assert not refs

    me = lax.axis_index("batch")
    here = {"y": lax.div(me, SIDE), "x": lax.rem(me, SIDE)}
    step = {a: {d: lax.rem(here[a] + d + SIDE, SIDE) for d in AWAY} for a in ("y", "x")}

    def device(axis, d):
        at = dict(here)
        at[axis] = step[axis][d]
        return {"batch": at["y"] * SIDE + at["x"]}


    def load(group, source, target):
        pltpu.make_async_copy(source, target, load_sem.at[group]).start()

    def loaded(group, size_of):
        pltpu.make_async_copy(size_of, size_of, load_sem.at[group]).wait()

    own_loads = 2 * len(SEGMENTS)
    norm_loads = ((grad_norm, norm_grad_in), (weight_norm, norm_weight_in), (moment_norm, norm_moment_in))

    def load_segment(half, s):
        at, count = segment_spans()[s]
        for k in range(at, at + count):
            name, part_no = PIECES[half][k]
            lanes = pl.ds(part_no * LANES, LANES)
            if name in ROW_CUT:
                load(half * len(SEGMENTS) + s, grad[name].at[0, :, lanes], landed[0].at[slot_of(half, k)])
            else:
                load(half * len(SEGMENTS) + s, grad[name].at[0, lanes, :], landed[1].at[slot_of(half, k)])

    def load_own():
        for n, (source, target) in enumerate(norm_loads):
            load(own_loads + 1 + n, source, target)
        for name in NAMES:
            load(own_loads, weight[name], weight_in[name])
            load(own_loads, moment[name], moment_in[name])

    for half in (0, 1):
        load_segment(half, 0)
    barrier = pltpu.get_barrier_semaphore()
    for axis in ("y", "x"):
        for d in (1, -1):
            pl.semaphore_signal(barrier, inc=1, device_id=device(axis, d), device_id_type=pl.DeviceIdType.MESH)

    def pack_piece(half, k):
        name, part_no = PIECES[half][k]
        rows = pl.ds(k * ROWS, ROWS)
        slot = slot_of(half, k)

        def put(b, value):
            y, x = divmod(b, SIDE)
            at = (y, x) if AXES[half][0] == "y" else (x, y)
            packed[half][at[0], at[1], rows, :] = value.astype(BF16)

        if name in ROW_CUT:
            for b in range(SIDE * SIDE):
                put(b, landed[0][slot, b * ROWS : (b + 1) * ROWS, :])
        else:
            for m in range(SIDE * SIDE // 2):
                lanes = slice(m * LANES, (m + 1) * LANES)
                pair = interleave(landed[1][slot, :ROWS, lanes], landed[1][slot, ROWS:, lanes])
                put(2 * m, pair[0])
                put(2 * m + 1, pair[1])

    def pack_own():
        loaded(own_loads, landed[0].at[0:3, 0 : SIDE * SIDE * ROWS // 2, :])
        for half in (0, 1):
            for k, (name, part_no) in enumerate(PIECES[half]):
                rows = pl.ds(k * ROWS, ROWS)
                for source, target in ((weight_in[name], weight_packed[half]), (moment_in[name], moment_packed[half])):
                    if name in ROW_CUT:
                        target[rows, :] = source[:, part_no * LANES : (part_no + 1) * LANES]
                    else:
                        turned = source[:, part_no * LANES : (part_no + 1) * LANES].T
                        target[rows, :] = jnp.concatenate([turned[:ROWS, :], turned[ROWS:, :]], axis=1)

    def remote(source, target, axis, d, group, slot):
        return pltpu.make_async_remote_copy(
            src_ref=source,
            dst_ref=target,
            send_sem=send_sem.at[group],
            recv_sem=recv_sem.at[slot],
            device_id=device(axis, d),
            device_id_type=pl.DeviceIdType.MESH,
        )

    def slot_at(half, s, kind):
        return (half * len(SEGMENTS) + s) * ARRIVALS + kind

    norm_slots = {"y": slot_at(2, 0, 0), "x": slot_at(2, 0, 1)}

    def arrived(slot, size_of):
        remote(size_of, size_of, "y", 1, 0, slot).wait_recv()

    def all_sent(group, size_of):
        remote(size_of, size_of, "y", 1, group, 0).wait_send()

    def spans(s):
        at, count = segment_spans()[s]
        rows, side = at * ROWS, count * ROWS // 2
        return (pl.ds(rows, side), pl.ds(rows + side, side), pl.ds(rows // 2, side), pl.ds(rows, 2 * side))

    def first_send(half, s):
        axis = AXES[half][0]
        low, high, place, _ = spans(s)
        data, land = packed[half], from_1[half]
        group, near, far = half * 4, slot_at(half, s, 0), slot_at(half, s, 1)
        for source, rows, kind, side, d, slot in (
            (2, low, 0, 0, 1, near),
            (2, high, 0, 1, -1, near),
            (1, high, 1, 0, 1, far),
            (-1, low, 1, 1, -1, far),
        ):
            remote(data.at[step[axis][source], :, rows, :], land.at[kind, side, :, place, :], axis, d, group, slot).start()

    def first_forward(half, s):
        axis = AXES[half][0]
        low, high, place, _ = spans(s)
        data, land = packed[half], from_1[half]
        arrived(slot_at(half, s, 0), land.at[0, :, :, place, :])
        for side, d, rows in ((0, 1, low), (1, -1, high)):
            to = step[axis][d]
            total = data[to, :, rows, :].astype(F32) + land[0, side, :, place, :].astype(F32)
            data[to, :, rows, :] = total.astype(BF16)
            target = land.at[2, side, :, place, :]
            remote(data.at[to, :, rows, :], target, axis, d, half * 4, slot_at(half, s, 1)).start()

    def second_send(half, s):
        low, high, place, whole = spans(s)
        data, land = packed[half], from_1[half]
        arrived(slot_at(half, s, 1), land.at[1:3, :, :, place, :])
        mine = here[AXES[half][0]]
        for rows, first, second in ((low, 2, 1), (high, 1, 2)):
            total = data[mine, :, rows, :].astype(F32)
            total += land[first, 0, :, place, :].astype(F32)
            total += land[second, 1, :, place, :].astype(F32)
            part[half][:, rows, :] = total.astype(BF16)
        axis = AXES[half][1]
        for n, d in ((2, 2), (0, 1), (1, -1)):
            source, target = part[half].at[step[axis][d], whole, :], from_2[half].at[n, whole, :]
            remote(source, target, axis, d, half * 4 + 1, slot_at(half, s, 2)).start()

    mean_rate = float(SIDE * SIDE) ** -0.5

    def update(half, s, far):
        first, second = AXES[half]
        whole = spans(s)[3]
        arrived(slot_at(half, s, 2), from_2[half].at[:, whole, :])
        total = part[half][here[second], whole, :].astype(F32)
        for n in range(3):
            total += from_2[half][n, whole, :].astype(F32)
        state = hold_rate * moment_packed[half][whole, :] + total * mean_rate
        new = weight_packed[half][whole, :] - learn_rate * state
        state_rows[half][whole, :] = state
        new_rows[half][whole, :] = new
        full[half][here[first], here[second], whole, :] = new.astype(BF16)
        own = full[half].at[here[first], here[second], whole, :]
        for d in (2, 1, -1) if far else (1, -1):
            remote(own, own, second, d, half * 4 + 2, slot_at(half, s, 3)).start()
        if not far:
            share_block(half, s, 0)

    def turn_own(half, s):
        at, count = segment_spans()[s]
        for k in range(at, at + count):
            name, part_no = PIECES[half][k]
            if name in ROW_CUT:
                continue
            rows = pl.ds(k * ROWS, ROWS)
            targets = (new_down, state_down) if name == "down" else (new_mixed, state_mixed)
            for source, target in zip((new_rows[half], state_rows[half]), targets):
                turned = source[rows, :].T
                target[:, part_no * LANES : (part_no + 1) * LANES] = jnp.concatenate([turned[:ROWS, :], turned[ROWS:, :]], axis=1)

    def share_block(half, s, away):
        first, second = AXES[half]
        at = step[second][away] if away else here[second]
        block = full[half].at[here[first], at, spans(s)[3], :]
        for d in (1, -1):
            remote(block, block, first, d, half * 4 + 3, slot_at(half, s, 5)).start()

    def share_all(half, s):
        first = AXES[half][0]
        whole = spans(s)[3]
        arrived(slot_at(half, s, 3), full[half].at[0, 0:3, whole, :])
        block = full[half].at[here[first], :, whole, :]
        for d in (1, -1):
            remote(block, block, first, d, half * 4 + 3, slot_at(half, s, 5)).start()
        turn_own(half, s)

    def share(half, s):
        first, second = AXES[half]
        low, high, _, whole = spans(s)
        arrived(slot_at(half, s, 3), full[half].at[0, 0:2, whole, :])
        for d, rows in ((1, low), (-1, high)):
            block = full[half].at[here[first], step[second][-d], rows, :]
            remote(block, block, second, d, half * 4 + 2, slot_at(half, s, 4)).start()
        for away in (1, -1):
            share_block(half, s, away)
        turn_own(half, s)

    def share_last(half, s):
        arrived(slot_at(half, s, 4), full[half].at[0, 0, spans(s)[3], :])
        share_block(half, s, 2)

    def share_forward(half, s):
        first = AXES[half][0]
        low, high, _, whole = spans(s)
        arrived(slot_at(half, s, 5), full[half].at[0:2, :, whole, :])
        for d, rows in ((1, low), (-1, high)):
            block = full[half].at[step[first][-d], :, rows, :]
            remote(block, block, first, d, half * 4 + 3, slot_at(half, s, 6)).start()

    def unpack(half, s):
        at, count = segment_spans()[s]
        for k in range(at, at + count):
            name, part_no = PIECES[half][k]
            if name in ROW_CUT:
                continue
            target = full_down if name == "down" else full_mixed
            rows = pl.ds(k * ROWS, ROWS)
            for m in range(SIDE * SIDE // 2):
                pair = []
                for b in (2 * m, 2 * m + 1):
                    y, x = divmod(b, SIDE)
                    at_ = (y, x) if AXES[half][0] == "y" else (x, y)
                    pair.append(full[half][at_[0], at_[1], rows, :].astype(F32))
                top, bottom = interleave(*pair)
                lanes = slice(m * LANES, (m + 1) * LANES)
                target[part_no * LANES : part_no * LANES + ROWS, lanes] = top.astype(BF16)
                target[part_no * LANES + ROWS : (part_no + 1) * LANES, lanes] = bottom.astype(BF16)

    def norm_start():
        for n, (_, target) in enumerate(norm_loads):
            loaded(own_loads + 1 + n, target)
        for k in range(8):
            norm_tiles[0, k : k + 1, :] = norm_grad_in[0:1, k * LANES : (k + 1) * LANES]
        base = norm_weight_in[...] - learn_rate * (hold_rate * norm_moment_in[...])
        base = jnp.broadcast_to(jnp.concatenate([base, base], axis=1), (8, LANES))
        row = lax.broadcasted_iota(jnp.int32, (8, LANES), 0)
        owner = 2 * row + jnp.where(low_lanes((8, LANES)), 0, 1)
        norm_tiles[0, 8:16, :] = jnp.where(owner == me, base, 0.0)
        norm_send("y", 0)

    def norm_send(axis, at):
        for n, d in enumerate(AWAY):
            remote(norm_tiles.at[at], norm_tiles.at[at + 1 + n], axis, d, 8, norm_slots[axis]).start()

    def norm_total(axis, at):
        arrived(norm_slots[axis], norm_tiles.at[at + 1 : at + 4])
        return (norm_tiles[at] + norm_tiles[at + 1]) + (norm_tiles[at + 2] + norm_tiles[at + 3])

    def norm_middle():
        norm_tiles[4] = norm_total("y", 0)
        norm_send("x", 4)

    def norm_end():
        total = norm_total("x", 4)
        mean = total[0:8, :] * mean_rate
        norm_tiles[8, 0:8, :] = mean
        new = (total[8:16, :] - learn_rate * mean).astype(BF16)
        for k in range(8):
            copy_norm[k * LANES : (k + 1) * LANES] = new[k, :]
        own = norm_tiles[8, pl.ds(lax.div(me, 2), 1), :]
        own = jnp.where(lax.rem(me, 2) == 1, swap_sides(own), own)[:, : LANES // 2]
        state = hold_rate * norm_moment_in[...] + own
        state_norm[...] = state
        new_norm[...] = norm_weight_in[...] - learn_rate * state

    def begin(half, s):
        at, count = segment_spans()[s]
        loaded(half * len(SEGMENTS) + s, landed[0].at[0:count])
        for k in range(at, at + count):
            pack_piece(half, k)
        if half == 0 and s == 0:
            pl.semaphore_wait(barrier, 4)
        first_send(half, s)
        if s + 1 < len(SEGMENTS):
            load_segment(half, s + 1)
        elif half == 1:
            load_own()

    def finish(half, s):
        arrived(slot_at(half, s, 6), full[half].at[0, :, spans(s)[3], :])
        unpack(half, s)

    def run(order, far=False):
        stages = dict(
            B=begin,
            F=first_forward,
            T=second_send,
            U=lambda half, s: update(half, s, far),
            S=share_all if far else share,
            L=share_last,
            G=share_forward,
            E=finish,
        )
        extras = dict(N=norm_start, M=norm_middle, O=pack_own, X=norm_end)
        for name in order:
            if name in extras:
                extras[name]()
            else:
                for half in (0, 1):
                    stages[name[0]](half, int(name[1]))

    run(REDUCE)
    core = lax.rem(lax.axis_index("cols"), 2)
    pl.when(core == 0)(lambda: run(GATHER_FAR, far=True))
    pl.when(core == 1)(lambda: run(GATHER_NEAR))
    for half in (0, 1):
        for n, size_of in enumerate((from_1[half], from_2[half], from_2[half], from_1[half])):
            all_sent(half * 4 + n, size_of)
    all_sent(8, norm_tiles.at[0:6])


def slot_of(half, k):
    order = [p for h in (0, 1) for p in PIECES[h]]
    this = PIECES[half][k]
    kind = this[0] in ROW_CUT
    return [p for p in order if (p[0] in ROW_CUT) == kind].index(this)


def place_kernel(*refs):
    refs = list(refs)

    def take(count):
        got, refs[:] = refs[:count], refs[count:]
        return got

    full = take(2)
    full_down, full_mixed = take(2)
    new_rows, state_rows = take(2), take(2)
    new_down_in, state_down_in, new_mixed_in, state_mixed_in = take(4)
    norms_in = take(3)
    copy_out = dict(zip(ROW_CUT, take(4)))
    copy_down, copy_mixed = take(2)
    new_out = dict(zip(ROW_CUT, take(4)))
    new_down, new_mixed = take(2)
    state_out = dict(zip(ROW_CUT, take(4)))
    state_down, state_mixed = take(2)
    norms_out = take(3)
    (sem,) = take(1)
    assert not refs

    def put(source, target, group):
        pltpu.make_async_copy(source, target, sem.at[group]).start()

    for half in (0, 1):
        for k, (name, part_no) in enumerate(PIECES[half]):
            if name not in ROW_CUT:
                continue
            rows, lanes = pl.ds(k * ROWS, ROWS), pl.ds(part_no * LANES, LANES)
            if AXES[half][0] == "y":
                put(full[half].at[:, :, rows, :], copy_out[name].at[:, :, :, lanes], 0)
            else:
                for n in range(SIDE):
                    put(full[half].at[n, :, rows, :], copy_out[name].at[:, n, :, lanes], 1)
            put(new_rows[half].at[rows, :], new_out[name].at[:, lanes], 2)
            put(state_rows[half].at[rows, :], state_out[name].at[:, lanes], 2)
    put(full_down, copy_down, 1)
    put(full_mixed, copy_mixed, 1)
    put(new_down_in, new_down, 2)
    put(state_down_in, state_down, 2)
    put(new_mixed_in, new_mixed, 2)
    put(state_mixed_in, state_mixed, 2)
    for n, (source, target) in enumerate(zip(norms_in, norms_out)):
        put(source, target, 3 + n)
    for group, size_of in enumerate((full[0], full[1], full[0].at[0:2], *norms_in)):
        pltpu.make_async_copy(size_of, size_of, sem.at[group]).wait()


def in_hbm(arrays):
    return [pltpu.with_memory_space_constraint(a, pltpu.HBM) for a in arrays]


def body(*arrays):
    arrays = [a.T if a.ndim == 2 and a.shape[1] == ROWS else a for a in arrays]
    grads, weights, moments = arrays[:7], arrays[7:14], arrays[14:]
    shapes = [w.shape for w in weights[:6]]
    half = jax.ShapeDtypeStruct((SIDE, SIDE, HALF_ROWS, LANES), BF16)
    rows = jax.ShapeDtypeStruct((HALF_ROWS, LANES), F32)
    down, mixed = jax.ShapeDtypeStruct(shapes[1], F32), jax.ShapeDtypeStruct(shapes[5], F32)
    held = (
        half,
        half,
        jax.ShapeDtypeStruct(grads[1].shape[1:], BF16),
        jax.ShapeDtypeStruct(grads[5].shape[1:], BF16),
        rows,
        rows,
        rows,
        rows,
        down,
        down,
        mixed,
        mixed,
        jax.ShapeDtypeStruct((8 * LANES,), BF16),
        jax.ShapeDtypeStruct((1, LANES // 2), F32),
        jax.ShapeDtypeStruct((1, LANES // 2), F32),
    )
    dma = pltpu.SemaphoreType.DMA
    remote = 2 * len(SEGMENTS) * ARRIVALS + 2
    vmem = pl.BlockSpec(memory_space=pltpu.VMEM)
    anywhere = pl.BlockSpec(memory_space=pltpu.HBM)
    half_scratch = pltpu.VMEM((SIDE, SIDE, HALF_ROWS, LANES), BF16)
    part_scratch = pltpu.VMEM((SIDE, HALF_ROWS, LANES), BF16)
    from_1 = pltpu.VMEM((3, 2, SIDE, HALF_ROWS // 2, LANES), BF16)
    from_2 = pltpu.VMEM((3, HALF_ROWS, LANES), BF16)
    own = [pltpu.VMEM(s, F32) for s in shapes]
    own_packed = pltpu.VMEM((HALF_ROWS, LANES), F32)
    small = pltpu.VMEM((1, LANES // 2), F32)
    results = pl.pallas_call(
        exchange_kernel,
        out_shape=held,
        in_specs=[anywhere] * 21,
        out_specs=[vmem] * len(held),
        scratch_shapes=[
            pltpu.VMEM((7, SIDE * SIDE * ROWS, LANES), F32),
            pltpu.VMEM((5, LANES, SIDE * SIDE * ROWS), F32),
            half_scratch,
            half_scratch,
            part_scratch,
            part_scratch,
            from_1,
            from_1,
            from_2,
            from_2,
            *own,
            *own,
            own_packed,
            own_packed,
            own_packed,
            own_packed,
            pltpu.VMEM((1, 8 * LANES), F32),
            small,
            small,
            pltpu.VMEM((9, 16, LANES), F32),
            dma((2 * len(SEGMENTS) + 4,)),
            dma((SENT_GROUPS,)),
            dma((remote,)),
        ],
        compiler_params=pltpu.CompilerParams(
            collective_id=0, has_side_effects=True, vmem_limit_bytes=32 * 1024 * 1024
        ),
        name="exchange",
    )(
        *in_hbm(grads),
        *in_hbm(weights[:6]),
        *in_hbm([weights[6].reshape(1, -1)]),
        *in_hbm(moments[:6]),
        *in_hbm([moments[6].reshape(1, -1)]),
    )
    row_shapes = [shapes[NAMES.index(n)] for n in ROW_CUT]
    tall = [jax.ShapeDtypeStruct((SIDE, SIDE, *s), BF16) for s in row_shapes]
    own_rows = [jax.ShapeDtypeStruct(s, F32) for s in row_shapes]
    placed = pl.pallas_call(
        place_kernel,
        out_shape=(*tall, held[2], held[3], *own_rows, down, mixed, *own_rows, down, mixed, *held[12:]),
        in_specs=[vmem] * 15,
        out_specs=[anywhere] * 21,
        scratch_shapes=[dma((6,))],
        compiler_params=pltpu.CompilerParams(vmem_limit_bytes=16 * 1024 * 1024),
        name="place",
    )(*results)
    outs = []
    for k, last in zip((0, 6, 12), placed[18:]):
        up, query, key, value, down_, mixed_ = placed[k : k + 6]
        group = [up, down_, query, key, value, mixed_]
        if k == 0:
            group = [g.reshape(-1, g.shape[-1]) for g in group]
        else:
            group[1], group[5] = group[1].T, group[5].T
        outs += [*group, last.reshape(-1)]
    return tuple(outs)


def solution(mesh):
    cut_rows, cut_columns = P("batch", "cols"), P("cols", "batch")
    own = (cut_rows, cut_columns, cut_rows, cut_rows, cut_rows, cut_columns, P("batch"))
    grad_rows, grad_columns = P("batch", None, "cols"), P("batch", "cols", None)
    grads = (grad_rows, grad_columns, grad_rows, grad_rows, grad_rows, grad_columns, P("batch", None))
    whole_rows, whole_columns = P(None, "cols"), P("cols", None)
    copies = (whole_rows, whole_columns, whole_rows, whole_rows, whole_rows, whole_columns, P())
    return jax.shard_map(
        body, mesh=mesh, in_specs=(*grads, *own, *own), out_specs=(*copies, *own, *own), check_vma=False
    )
```
